32 devices in a mesh: comp: 2 (over core), lat: 4 (over z), lon: 4 (over y, x).
Axes of the slice: x: 2, y: 2, z: 4, core: 2. Of those that a mesh axis runs over, the one named last changes fastest.
Arguments:
- fields: float32 [2, 7, 2048, 256], P('comp', None, ('lat', 'lon')), may hold values from -4 to 4, as said below
- block_owner: int32 [2048], P(('lat', 'lon')), may hold values from 0 to 2047, as said below
- ice_covered: int32 [2048], P(('lat', 'lon')), may hold values 0 or 1
- land_mask: int32 [2048, 256], P(('lat', 'lon')), may hold values 0 or 1
Outputs:
- coupled_out: float32 [2, 2, 2048, 256], P('comp', None, ('lat', 'lon'))
The draws below stay inside these ranges and needn't reach their ends.
Inputs may be any that keep to these rules, and one draw needn't show every extreme that they name: `block_owner`: every block id appears once. Slot d of lat+lon index o holds a block of the ice tile of index d, that is an id from d * 128 to d * 128 + 127. `fields`: ocean channels: winds within 4, currents within 1.5, tilts within 1, air density 0.9 to 1.3; ice channels: velocities within 1.5, mass 0.5 to 4, concentration 0.05 to 1, stresses within 1.5.
All inputs are finite; a program needn't handle non-finite values.
Results may differ from the reference program's by a relative error of at most 0.00002.
Values sent between devices are 32-bit elements.
A program may use at most 64 MiB of HBM per device.

```python
import jax
import jax.numpy as jnp

KB = 128
GX = 1
BY = 2
BX = 128
NSUB = 4
NBALL = 2048
CELLS = 256
N_LAT = 4
N_LON = 4


def clipped_normal(subkey, scale, limit):
    return jnp.clip(scale * jax.random.normal(subkey, (NBALL, CELLS), jnp.float32), -limit, limit)


def uniform_draw(subkey, low, high):
    return jax.random.uniform(subkey, (NBALL, CELLS), jnp.float32, low, high)


def draw_fields(key, part):
    subkeys = jax.random.split(jax.random.fold_in(key, 11), 14)
    wind = [clipped_normal(subkeys[0], 1.5, 4.0), clipped_normal(subkeys[1], 1.5, 4.0)]
    current = [clipped_normal(subkeys[2], 0.5, 1.5), clipped_normal(subkeys[3], 0.5, 1.5)]
    tilt = [clipped_normal(subkeys[4], 0.3, 1.0), clipped_normal(subkeys[5], 0.3, 1.0)]
    drift = [clipped_normal(subkeys[7], 0.5, 1.5), clipped_normal(subkeys[8], 0.5, 1.5)]
    concentration = uniform_draw(subkeys[10], 0.05, 1.0)
    stresses = [clipped_normal(subkeys[11], 0.5, 1.5), clipped_normal(subkeys[12], 0.5, 1.5), clipped_normal(subkeys[13], 0.5, 1.5)]
    density = uniform_draw(subkeys[6], 0.9, 1.3)
    ice_mass = jnp.exp(uniform_draw(subkeys[9], jnp.log(0.5), jnp.log(4.0)))
    ocean = jnp.stack(wind + current + tilt + [density])
    sea_ice = jnp.stack(drift + [ice_mass, concentration] + stresses)
    return jnp.stack([ocean, sea_ice]).astype(jnp.float32)


def draw_block_owner(key, part):
    devices = N_LAT * N_LON
    per_peer = KB // devices
    subkeys = jax.random.split(jax.random.fold_in(key, 5), devices)
    orders = jax.vmap(lambda subkey: jax.random.permutation(subkey, KB))(subkeys)
    ids = orders.astype(jnp.int32) + (jnp.arange(devices, dtype=jnp.int32) * KB)[:, None]
    ids = ids.reshape(devices, devices, per_peer).transpose(1, 0, 2)
    return ids.reshape(devices * KB).astype(jnp.int32)


def plant(array, key, smallest, largest):
    extent = array.shape
    place = [jax.random.randint(jax.random.fold_in(key, axis), (), 0, extent[axis]) for axis in range(len(extent))]
    array = array.at[tuple(place)].set(smallest)
    longest = extent.index(max(extent))
    place[longest] = (place[longest] + 1) % extent[longest]
    return array.at[tuple(place)].set(largest)


def setup_inputs(seed: int = 0) -> dict:
    streams_of = jax.random.split(jax.random.key(seed), 5)
    fields = draw_fields(jax.random.fold_in(streams_of[4], 71), 0)
    block_owner = draw_block_owner(jax.random.fold_in(streams_of[4], 71), 0)
    ice_covered = plant((jax.random.randint(streams_of[2], (NBALL,), 0, 4) < 3).astype(jnp.int32), jax.random.fold_in(streams_of[2], 1), 0, 1)
    land_mask = plant((jax.random.randint(streams_of[3], (NBALL, CELLS), 0, 8) < 1).astype(jnp.int32), jax.random.fold_in(streams_of[3], 1), 0, 1)
    return dict(fields=fields, block_owner=block_owner, ice_covered=ice_covered, land_mask=land_mask)


CD_ICE = 0.1
CW = 1.5
CSTAR = 2.0
ECC2 = 4.0
DMIN2 = 0.25
RELAX = 0.5
DTE = 0.5
CORIO = 0.3
MASS_FLOOR = 0.5
DRAG_FLOOR = 0.1

def air_stress(ocean):
    wind_x, wind_y, current_x, current_y, tilt_x, tilt_y, density = ocean
    speed_ice = jnp.sqrt(wind_x * wind_x + wind_y * wind_y + 1.0)
    scale_ice = density * CD_ICE * speed_ice
    rel_x = wind_x - current_x
    rel_y = wind_y - current_y
    speed_open = jnp.sqrt(rel_x * rel_x + rel_y * rel_y + 1.0)
    scale_open = density * (0.1 + 0.05 * speed_open) * speed_open
    outbound = jnp.stack([scale_ice * wind_x, scale_ice * wind_y, current_x, current_y, tilt_x, tilt_y])
    open_stress = jnp.stack([scale_open * rel_x, scale_open * rel_y])
    return (outbound, open_stress)

def prepare(ice_tile, forcing, active):
    ice_mass = ice_tile[2]
    concentration = ice_tile[3]
    strength = ice_mass * jnp.exp(CSTAR * (concentration - 1.0)) * active
    drag_base = CW * concentration * active
    push_x = active * (concentration * forcing[0] - ice_mass * forcing[4])
    push_y = active * (concentration * forcing[1] - ice_mass * forcing[5])
    return jnp.stack([strength, ice_mass, drag_base, push_x, push_y, forcing[2], forcing[3], active])

def subcycle(ice_state, statics):
    east_vel, north_vel, stress_one, stress_two, stress_three = ice_state
    strength = statics[0]
    east_base = east_vel[:-1, :-1]
    north_base = north_vel[:-1, :-1]
    strain_xx = east_vel[:-1, 1:] - east_base
    strain_yy = north_vel[1:, :-1] - north_base
    shear = east_vel[1:, :-1] - east_base + (north_vel[:-1, 1:] - north_base)
    divergence = strain_xx + strain_yy
    tension = strain_xx - strain_yy
    delta_norm = jnp.sqrt(divergence * divergence + (tension * tension + shear * shear) / ECC2 + DMIN2)
    viscosity = strength[:-1, :-1] / delta_norm
    stress_sum = (stress_one[:-1, :-1] + RELAX * viscosity * (divergence - delta_norm)) / (1.0 + RELAX)
    stress_diff = (stress_two[:-1, :-1] + RELAX * viscosity * tension / ECC2) / (1.0 + RELAX)
    stress_shear = (stress_three[:-1, :-1] + RELAX * viscosity * shear / (2.0 * ECC2)) / (1.0 + RELAX)
    stress_xx = 0.5 * (stress_sum + stress_diff)
    stress_yy = 0.5 * (stress_sum - stress_diff)
    force_x = stress_xx[1:, 1:] - stress_xx[1:, :-1] + (stress_shear[1:, 1:] - stress_shear[:-1, 1:])
    force_y = stress_shear[1:, 1:] - stress_shear[1:, :-1] + (stress_yy[1:, 1:] - stress_yy[:-1, 1:])
    trimmed = statics[:, 1:-1, 1:-1]
    strength, ice_mass, drag_base, push_x, push_y, current_x, current_y, active = trimmed
    east_old = east_vel[1:-1, 1:-1]
    north_old = north_vel[1:-1, 1:-1]
    diff_x = current_x - east_old
    diff_y = current_y - north_old
    drag_coef = drag_base * jnp.sqrt(diff_x * diff_x + diff_y * diff_y + DRAG_FLOOR)
    denominator = jnp.maximum(ice_mass, MASS_FLOOR) / DTE + drag_coef
    east_new = active * (ice_mass / DTE * east_old + force_x + push_x + drag_coef * current_x + CORIO * ice_mass * north_old) / denominator
    north_new = active * (ice_mass / DTE * north_old + force_y + push_y + drag_coef * current_y - CORIO * ice_mass * east_old) / denominator
    new_state = jnp.stack([east_new, north_new, stress_sum[1:, 1:], stress_diff[1:, 1:], stress_shear[1:, 1:]])
    return (new_state, trimmed)

def give_back(ice_state, statics):
    east_vel = ice_state[0]
    north_vel = ice_state[1]
    drag_base = statics[2]
    current_x = statics[5]
    current_y = statics[6]
    diff_x = east_vel - current_x
    diff_y = north_vel - current_y
    factor = drag_base * jnp.sqrt(diff_x * diff_x + diff_y * diff_y + DRAG_FLOOR)
    return jnp.stack([factor * diff_x, factor * diff_y, drag_base / CW])

def to_grid(blocks):
    channels = blocks.shape[0]
    arranged = blocks.reshape(channels, N_LAT, N_LON, KB // GX, GX, BY, BX)
    arranged = arranged.transpose(0, 1, 3, 5, 2, 4, 6)
    return arranged.reshape(channels, N_LAT * (KB // GX) * BY, N_LON * GX * BX)

def from_grid(values):
    channels = values.shape[0]
    arranged = values.reshape(channels, N_LAT, KB // GX, BY, N_LON, GX, BX)
    arranged = arranged.transpose(0, 1, 4, 2, 5, 3, 6)
    return arranged.reshape(channels, N_LAT * N_LON * KB, BY * BX)

def extend_grid(values, width):
    values = jnp.concatenate([values[..., -width:], values, values[..., :width]], axis=-1)
    return jnp.pad(values, ((0, 0), (width, width), (0, 0)))

def reference(fields, block_owner, ice_covered, land_mask):
    outbound, open_stress = air_stress(fields[0])
    geographic = jnp.zeros_like(outbound).at[:, block_owner].set(outbound)
    forcing = to_grid(geographic)
    ice_tile = to_grid(fields[1])
    covered = ice_covered.astype(jnp.float32)[:, None] * (1 - land_mask).astype(jnp.float32)
    active = to_grid(covered[None])[0]
    statics = prepare(ice_tile, forcing, active)
    ice_state = jnp.stack([ice_tile[0], ice_tile[1], ice_tile[4], ice_tile[5], ice_tile[6]])
    ice_state = extend_grid(ice_state, NSUB)
    statics = extend_grid(statics, NSUB)
    for repeat in range(NSUB):
        ice_state, statics = subcycle(ice_state, statics)
    returned = from_grid(give_back(ice_state, statics))
    received_back = returned[:, block_owner]
    ocean_out = received_back[:2] + (1.0 - received_back[2]) * open_stress
    ice_out = from_grid(ice_state[:2])
    return jnp.stack([ocean_out, ice_out])
```

```python
import functools

import jax
import jax.numpy as jnp
from jax import lax
from jax.experimental import pallas as pl
from jax.experimental.pallas import tpu as pltpu
from jax.sharding import PartitionSpec as P

GX = 1
BY = 2
BX = 128
NSUB = 4


CD_ICE = 0.1
CW = 1.5
CSTAR = 2.0
ECC2 = 4.0
DMIN2 = 0.25
RELAX = 0.5
DTE = 0.5
CORIO = 0.3
MASS_FLOOR = 0.5
DRAG_FLOOR = 0.1


def from_behind(x, axis, by):
    size = lax.axis_size(axis)
    pairs = [(i, i + by) for i in range(size) if 0 <= i + by < size]
    return lax.ppermute(x, axis, pairs)


def with_halo(x, sides, width, wrap):
    for axis, dim in sides:
        size, length = (lax.axis_size(axis), x.shape[dim])
        up = [(i, (i + 1) % size) for i in range(size if wrap else size - 1)]
        down = [(j, i) for i, j in up]
        last = lax.slice_in_dim(x, length - width, length, axis=dim)
        first = lax.slice_in_dim(x, 0, width, axis=dim)
        before = lax.ppermute(last, axis, up)
        after = lax.ppermute(first, axis, down)
        x = jnp.concatenate([before, x, after], axis=dim)
    return x


def air_stress(ocean):
    wind_x, wind_y, current_x, current_y, tilt_x, tilt_y, density = ocean
    speed_ice = jnp.sqrt(wind_x * wind_x + wind_y * wind_y + 1.0)
    scale_ice = density * CD_ICE * speed_ice
    rel_x = wind_x - current_x
    rel_y = wind_y - current_y
    speed_open = jnp.sqrt(rel_x * rel_x + rel_y * rel_y + 1.0)
    scale_open = density * (0.1 + 0.05 * speed_open) * speed_open
    outbound = jnp.stack(
        [scale_ice * wind_x, scale_ice * wind_y, current_x, current_y, tilt_x, tilt_y]
    )
    open_stress = jnp.stack([scale_open * rel_x, scale_open * rel_y])
    return (outbound, open_stress)


def prepare(ice_tile, forcing, active):
    ice_mass = ice_tile[2]
    concentration = ice_tile[3]
    strength = ice_mass * jnp.exp(CSTAR * (concentration - 1.0)) * active
    drag_base = CW * concentration * active
    push_x = active * (concentration * forcing[0] - ice_mass * forcing[4])
    push_y = active * (concentration * forcing[1] - ice_mass * forcing[5])
    return jnp.stack(
        [strength, ice_mass, drag_base, push_x, push_y, forcing[2], forcing[3], active]
    )


def subcycle(ice_state, statics):
    east_vel, north_vel, stress_one, stress_two, stress_three = ice_state
    strength = statics[0]
    east_base = east_vel[:-1, :-1]
    north_base = north_vel[:-1, :-1]
    strain_xx = east_vel[:-1, 1:] - east_base
    strain_yy = north_vel[1:, :-1] - north_base
    shear = east_vel[1:, :-1] - east_base + (north_vel[:-1, 1:] - north_base)
    divergence = strain_xx + strain_yy
    tension = strain_xx - strain_yy
    delta_norm = jnp.sqrt(
        divergence * divergence + (tension * tension + shear * shear) / ECC2 + DMIN2
    )
    viscosity = strength[:-1, :-1] / delta_norm
    stress_sum = (stress_one[:-1, :-1] + RELAX * viscosity * (divergence - delta_norm)) / (
        1.0 + RELAX
    )
    stress_diff = (stress_two[:-1, :-1] + RELAX * viscosity * tension / ECC2) / (1.0 + RELAX)
    stress_shear = (stress_three[:-1, :-1] + RELAX * viscosity * shear / (2.0 * ECC2)) / (
        1.0 + RELAX
    )
    stress_xx = 0.5 * (stress_sum + stress_diff)
    stress_yy = 0.5 * (stress_sum - stress_diff)
    force_x = (
        stress_xx[1:, 1:] - stress_xx[1:, :-1] + (stress_shear[1:, 1:] - stress_shear[:-1, 1:])
    )
    force_y = (
        stress_shear[1:, 1:] - stress_shear[1:, :-1] + (stress_yy[1:, 1:] - stress_yy[:-1, 1:])
    )
    trimmed = statics[:, 1:-1, 1:-1]
    strength, ice_mass, drag_base, push_x, push_y, current_x, current_y, active = trimmed
    east_old = east_vel[1:-1, 1:-1]
    north_old = north_vel[1:-1, 1:-1]
    diff_x = current_x - east_old
    diff_y = current_y - north_old
    drag_coef = drag_base * jnp.sqrt(diff_x * diff_x + diff_y * diff_y + DRAG_FLOOR)
    denominator = jnp.maximum(ice_mass, MASS_FLOOR) / DTE + drag_coef
    east_new = (
        active
        * (
            ice_mass / DTE * east_old
            + force_x
            + push_x
            + drag_coef * current_x
            + CORIO * ice_mass * north_old
        )
        / denominator
    )
    north_new = (
        active
        * (
            ice_mass / DTE * north_old
            + force_y
            + push_y
            + drag_coef * current_y
            - CORIO * ice_mass * east_old
        )
        / denominator
    )
    new_state = jnp.stack(
        [east_new, north_new, stress_sum[1:, 1:], stress_diff[1:, 1:], stress_shear[1:, 1:]]
    )
    return (new_state, trimmed)


def give_back(ice_state, statics):
    east_vel = ice_state[0]
    north_vel = ice_state[1]
    drag_base = statics[2]
    current_x = statics[5]
    current_y = statics[6]
    diff_x = east_vel - current_x
    diff_y = north_vel - current_y
    factor = drag_base * jnp.sqrt(diff_x * diff_x + diff_y * diff_y + DRAG_FLOOR)
    return jnp.stack([factor * diff_x, factor * diff_y, drag_base / CW])


def to_tile(blocks):
    channels, count, cells = blocks.shape
    arranged = blocks.reshape(channels, count // GX, GX, BY, BX).transpose(0, 1, 3, 2, 4)
    return arranged.reshape(channels, count // GX * BY, GX * BX)


def from_tile(values):
    channels, rows, columns = values.shape
    arranged = values.reshape(channels, rows // BY, BY, GX, BX).transpose(0, 1, 3, 2, 4)
    return arranged.reshape(channels, rows // BY * GX, BY * BX)


def per_device(fields, block_owner, ice_covered, land_mask):
    count = block_owner.shape[0]
    is_ocean = lax.axis_index("comp") == 0
    outbound, open_stress = air_stress(fields[0])
    owner_row = block_owner.reshape(1, count)
    crossed = from_behind(outbound, "comp", 1)
    received, anchor = (
        lax.all_to_all(crossed, ("lat", "lon"), split_axis=1, concat_axis=1, tiled=True),
        lax.all_to_all(owner_row, ("lat", "lon"), split_axis=1, concat_axis=1, tiled=True),
    )
    local_ids = anchor[0] % count
    position = jnp.zeros((count,), jnp.int32).at[local_ids].set(jnp.arange(count, dtype=jnp.int32))
    forcing = to_tile(received[:, position])
    ice_tile = to_tile(fields[0])
    covered = ice_covered.astype(jnp.float32)[:, None] * (1 - land_mask).astype(jnp.float32)
    active = to_tile(covered[None])[0]
    statics = prepare(ice_tile, forcing, active)
    ice_state = jnp.stack([ice_tile[0], ice_tile[1], ice_tile[4], ice_tile[5], ice_tile[6]])
    joined = jnp.concatenate([ice_state, statics], 0)
    joined = with_halo(joined, (("lon", 2),), NSUB, True)
    joined = with_halo(joined, (("lat", 1),), NSUB, False)
    ice_state = joined[:5]
    statics = joined[5:]
    for repeat in range(NSUB):
        ice_state, statics = subcycle(ice_state, statics)
    returned = from_tile(give_back(ice_state, statics))
    back_send = returned[:, local_ids]
    regrouped = lax.all_to_all(back_send, ("lat", "lon"), split_axis=1, concat_axis=1, tiled=True)
    received_back = from_behind(regrouped, "comp", -1)
    ocean_out = received_back[:2] + (1.0 - received_back[2]) * open_stress
    ice_out = from_tile(ice_state[:2])
    return jnp.where(is_ocean, ocean_out, ice_out)[None]


LEAD = 16
TILE = 8
MESH = pl.DeviceIdType.MESH
DIRECTIONS = [(a, b) for a in (-1, 0, 1) for b in (-1, 0, 1) if (a, b) != (0, 0)]
U, V, MASS, CONC, S1, S2, S12, ACTIVE, PUSH_X, PUSH_Y, CUR_X, CUR_Y = range(12)


def split_dot(one_hot, values, contract):
    total = None
    rest = values
    for piece in range(3):
        part = rest.astype(jnp.bfloat16)
        if piece < 2:
            rest = rest - part.astype(jnp.float32)
        term = lax.dot_general(
            one_hot, part, ((contract, (0,)), ((), ())), preferred_element_type=jnp.float32
        )
        total = term if total is None else total + term
    return total


def step_kernel(
    n_lat, n_lon,
    fields, owner, covered, land, out,
    surf, open_st, ret, ids, recv, grid, strength, dragb, forc, one_hot, back, land_v,
    pack_early, pack_late, got_early, got_late,
    load_sem, ids_ssem, ids_rsem, fwd_ssem, fwd_rsem, ret_ssem, ret_rsem,
    early_ssem, early_rsem, late_ssem, late_rsem,
):
    comp = lax.axis_index("comp")
    lat = lax.axis_index("lat")
    lon = lax.axis_index("lon")
    peers = n_lat * n_lon
    me = lat * n_lon + lon
    count = owner.shape[1]
    per = count // peers
    width = BX
    barrier = pltpu.get_barrier_semaphore()

    def rows_of(peer):
        return pl.ds(pl.multiple_of(peer * per, per), per)

    def device(kind, peer):
        return (kind, peer // n_lon, peer % n_lon)

    def each_peer(body):
        def step(k, carry):
            body((me + k) % peers)
            return carry
        lax.fori_loop(0, peers, step, 0)

    def signal_peers(kind):
        each_peer(
            lambda p: pl.semaphore_signal(
                barrier, inc=1, device_id=device(kind, p), device_id_type=MESH
            )
        )

    def send_rows(kind, src, lo, num, dst, dlo, ssem, rsem):
        def body(p):
            pltpu.make_async_remote_copy(
                src_ref=src.at[pl.ds(lo, num), rows_of(p), :],
                dst_ref=dst.at[pl.ds(dlo, num), rows_of(me), :],
                send_sem=ssem, recv_sem=rsem,
                device_id=device(kind, p), device_id_type=MESH,
            ).start()
        each_peer(body)

    def wait_bytes(ref, sem):
        pltpu.make_async_copy(ref, ref, sem).wait()

    @pl.when(comp == 0)
    def _ocean():
        raw = pltpu.make_async_copy(fields.at[0, pl.ds(2, 4)], surf.at[pl.ds(2, 4)], load_sem.at[0])
        wind = pltpu.make_async_copy(fields.at[0, pl.ds(0, 2)], surf.at[pl.ds(0, 2)], load_sem.at[1])
        rho = pltpu.make_async_copy(fields.at[0, pl.ds(6, 1)], surf.at[pl.ds(6, 1)], load_sem.at[2])
        raw.start()
        wind.start()
        rho.start()
        signal_peers(1)
        pl.semaphore_wait(barrier, peers)

        def ids_out(p):
            pltpu.make_async_remote_copy(
                src_ref=owner, dst_ref=ids.at[me], send_sem=ids_ssem, recv_sem=ids_rsem,
                device_id=device(1, p), device_id_type=MESH,
            ).start()
        each_peer(ids_out)
        raw.wait()
        send_rows(1, surf, 2, 4, recv, 2, fwd_ssem.at[0], fwd_rsem.at[0])
        wind.wait()
        rho.wait()

        def stress(t, carry):
            r = pl.ds(pl.multiple_of(t * TILE, TILE), TILE)
            wx, wy, density = surf[0, r, :], surf[1, r, :], surf[6, r, :]
            scale = density * CD_ICE * jnp.sqrt(wx * wx + wy * wy + 1.0)
            forc[0, r, :] = scale * wx
            forc[1, r, :] = scale * wy
            return carry
        lax.fori_loop(0, count // TILE, stress, 0)
        send_rows(1, forc, 0, 2, recv, 0, fwd_ssem.at[1], fwd_rsem.at[1])

        def open_water(t, carry):
            r = pl.ds(pl.multiple_of(t * TILE, TILE), TILE)
            density = surf[6, r, :]
            rel_x = surf[0, r, :] - surf[2, r, :]
            rel_y = surf[1, r, :] - surf[3, r, :]
            speed = jnp.sqrt(rel_x * rel_x + rel_y * rel_y + 1.0)
            scale = density * (0.1 + 0.05 * speed) * speed
            open_st[0, r, :] = scale * rel_x
            open_st[1, r, :] = scale * rel_y
            return carry
        lax.fori_loop(0, count // TILE, open_water, 0)
        wait_bytes(ret.at[pl.ds(2, 1)], ret_rsem.at[0])
        wait_bytes(ret.at[pl.ds(0, 2)], ret_rsem.at[1])

        def finish(t, carry):
            r = pl.ds(pl.multiple_of(t * TILE, TILE), TILE)
            water = 1.0 - ret[2, r, :]
            out[0, 0, r, :] = ret[0, r, :] + water * open_st[0, r, :]
            out[0, 1, r, :] = ret[1, r, :] + water * open_st[1, r, :]
            return carry
        lax.fori_loop(0, count // TILE, finish, 0)
        wait_bytes(ids, ids_ssem)
        wait_bytes(surf.at[pl.ds(2, 4)], fwd_ssem.at[0])
        wait_bytes(forc.at[pl.ds(0, 2)], fwd_ssem.at[1])

    @pl.when(comp == 1)
    def _ice():
        first, last = LEAD, LEAD + count
        core = pl.ds(first, count)
        main, side = pl.ds(0, width), pl.ds(width, width)
        loads = [
            pltpu.make_async_copy(
                fields.at[0, :, :, pl.ds(y * width, width)],
                grid.at[pl.ds(0, 7), y, core, main],
                load_sem.at[y],
            )
            for y in range(2)
        ]
        loads.append(pltpu.make_async_copy(land, land_v, load_sem.at[2]))
        for load in loads:
            load.start()
        for c in range(12):
            for y in range(2):
                blank = jnp.zeros((LEAD, 2 * width), jnp.float32)
                grid[c, y, pl.ds(0, LEAD), :] = blank
                grid[c, y, pl.ds(last, LEAD), :] = blank
        for got in (got_early, got_late):
            for d in range(2):
                got[d, pl.ds(0, TILE), :] = jnp.zeros((TILE, width), jnp.float32)
                got[d, pl.ds(TILE + count, TILE), :] = jnp.zeros((TILE, width), jnp.float32)

        def inside(a):
            if a == 0:
                return lat >= 0
            return lat + a >= 0 if a < 0 else lat + a < n_lat

        signal_peers(0)
        for a, b in DIRECTIONS:
            @pl.when(inside(a))
            def _():
                pl.semaphore_signal(
                    barrier, inc=1, device_id=(1, lat + a, (lon + b + n_lon) % n_lon),
                    device_id_type=MESH,
                )
        walls = jnp.where(lat == 0, 3, 0) + jnp.where(lat == n_lat - 1, 3, 0)
        pl.semaphore_wait(barrier, peers + 8 - walls)
        for load in loads:
            load.wait()

        diag = lax.broadcasted_iota(jnp.int32, (count, count), 0) == lax.broadcasted_iota(
            jnp.int32, (count, count), 1
        )
        wet = jnp.sum(
            jnp.where(diag, covered[...].astype(jnp.float32), 0.0), axis=1, keepdims=True
        )
        sea = wet * (1 - land_v[...]).astype(jnp.float32)
        for y in range(2):
            grid[ACTIVE, y, core, main] = sea[:, y * width:(y + 1) * width]

        lane = lax.broadcasted_iota(jnp.int32, (TILE, width), 1)

        def pack(lo, num, packed):
            def body(t, carry):
                r = pl.ds(pl.multiple_of(first + t * TILE, TILE), TILE)
                east = jnp.zeros((TILE, width), jnp.float32)
                west = east
                for c in range(num):
                    for y in range(2):
                        x = grid[lo + c, y, r, main]
                        slot = (c * 2 + y) * NSUB
                        mine = (lane >= slot) & (lane < slot + NSUB)
                        east = jnp.where(mine, pltpu.roll(x, (slot + NSUB) % width, 1), east)
                        west = jnp.where(mine, pltpu.roll(x, slot, 1) if slot else x, west)
                q = pl.ds(pl.multiple_of(t * TILE, TILE), TILE)
                packed[0, q, :] = east
                packed[1, q, :] = west
                return carry
            lax.fori_loop(0, count // TILE, body, 0)

        def halo(lo, num, packed, got, ssem, rsem, begin):
            for k, (a, b) in enumerate(DIRECTIONS):
                src_row = {-1: 0, 0: 0, 1: count - TILE}[a]
                dst_row = {-1: count, 0: 0, 1: -TILE}[a]
                rows = count if a == 0 else TILE
                if b == 0:
                    src = grid.at[pl.ds(lo, num), :, pl.ds(first + src_row, rows), main]
                    dst = grid.at[pl.ds(lo, num), :, pl.ds(first + dst_row, rows), main]
                else:
                    d = 0 if b > 0 else 1
                    src = packed.at[d, pl.ds(src_row, rows), :]
                    dst = got.at[d, pl.ds(TILE + dst_row, rows), :]
                copy = pltpu.make_async_remote_copy(
                    src_ref=src, dst_ref=dst, send_sem=ssem.at[k], recv_sem=rsem.at[k],
                    device_id=(1, lat + a, (lon + b + n_lon) % n_lon), device_id_type=MESH,
                )
                if begin:
                    @pl.when(inside(a))
                    def _():
                        copy.start()
                else:
                    @pl.when(inside(a))
                    def _():
                        copy.wait_send()

                    @pl.when(inside(-a))
                    def _():
                        copy.wait_recv()

        def side_of(got, slot, q):
            east = got[1, q, :]
            west = got[0, q, :]
            east = pltpu.roll(east, (width - slot) % width, 1) if slot else east
            west = pltpu.roll(west, width - NSUB - slot, 1)
            return jnp.where(
                lane < NSUB, east, jnp.where(lane >= width - NSUB, west, 0.0)
            )

        def unpack(lo, num, got, after):
            def body(t, carry):
                q = pl.ds(pl.multiple_of(t * TILE, TILE), TILE)
                r = pl.ds(pl.multiple_of(first + (t - 1) * TILE, TILE), TILE)
                for c in range(num):
                    for y in range(2):
                        grid[lo + c, y, r, side] = side_of(got, (c * 2 + y) * NSUB, q)
                after(r)
                return carry
            lax.fori_loop(0, count // TILE + 2, body, 0)

        pack(0, 8, pack_early)
        halo(0, 8, pack_early, got_early, early_ssem, early_rsem, True)

        def ice_statics(r):
            for y in range(2):
                conc = grid[CONC, y, r, :]
                act = grid[ACTIVE, y, r, :]
                strength[y, r, :] = grid[MASS, y, r, :] * jnp.exp(CSTAR * (conc - 1.0)) * act
                dragb[y, r, :] = CW * conc * act

        wait_bytes(ids, ids_rsem)
        wanted = me * per
        row_lane = lax.broadcasted_iota(jnp.int32, (per, count), 1)
        row_sub = lax.broadcasted_iota(jnp.int32, (per, count), 0)
        mine = row_lane == row_sub + wanted
        blocks = lax.broadcasted_iota(jnp.int32, (per, count), 1).astype(jnp.float32)
        base = (me * count).astype(jnp.float32)
        for p in range(peers):
            owned = jnp.broadcast_to(ids[p], (per, count)).astype(jnp.float32)
            local = jnp.sum(jnp.where(mine, owned, 0.0), axis=1, keepdims=True) - base
            one_hot[pl.ds(p * per, per), :] = jnp.where(local == blocks, 1.0, 0.0)

        halo(0, 8, pack_early, got_early, early_ssem, early_rsem, False)
        unpack(0, 8, got_early, ice_statics)

        perm = one_hot[...].astype(jnp.bfloat16)
        wait_bytes(recv.at[pl.ds(2, 4)], fwd_rsem.at[0])
        for c in range(2, 6):
            forc[c] = split_dot(perm, recv[c], (0,))
        wait_bytes(recv.at[pl.ds(0, 2)], fwd_rsem.at[1])
        for c in range(2):
            forc[c] = split_dot(perm, recv[c], (0,))

        def pushes(t, carry):
            q = pl.ds(pl.multiple_of(t * TILE, TILE), TILE)
            r = pl.ds(pl.multiple_of(first + t * TILE, TILE), TILE)
            for y in range(2):
                half = pl.ds(y * width, width)
                act, conc, mass = (grid[c, y, r, main] for c in (ACTIVE, CONC, MASS))
                grid[PUSH_X, y, r, main] = act * (conc * forc[0, q, half] - mass * forc[4, q, half])
                grid[PUSH_Y, y, r, main] = act * (conc * forc[1, q, half] - mass * forc[5, q, half])
                grid[CUR_X, y, r, main] = forc[2, q, half]
                grid[CUR_Y, y, r, main] = forc[3, q, half]
            return carry
        lax.fori_loop(0, count // TILE, pushes, 0)
        pack(PUSH_X, 4, pack_late)
        halo(PUSH_X, 4, pack_late, got_late, late_ssem, late_rsem, True)

        for y in range(2):
            share = grid[CONC, y, core, main] * grid[ACTIVE, y, core, main]
            back[2, :, pl.ds(y * width, width)] = split_dot(perm, share, (1,))
        send_rows(0, back, 2, 1, ret, 2, ret_ssem.at[0], ret_rsem.at[0])

        halo(PUSH_X, 4, pack_late, got_late, late_ssem, late_rsem, False)
        unpack(PUSH_X, 4, got_late, lambda r: None)

        def east_of(x):
            return pltpu.roll(x, 2 * width - 1, 1)

        def west_of(x):
            return pltpu.roll(x, 1, 1)

        sub = lax.broadcasted_iota(jnp.int32, (TILE, 2 * width), 0)

        def next_row(x, after):
            return pltpu.roll(jnp.where(sub == 0, after, x), TILE - 1, 0)

        def last_row(x, before):
            return pltpu.roll(jnp.where(sub == TILE - 1, before, x), 1, 0)

        def sweep(t):
            base_row = pl.multiple_of(first - TILE + t * TILE, TILE)
            r = pl.ds(base_row, TILE)
            nxt = pl.ds(pl.multiple_of(base_row + TILE, TILE), TILE)
            prev = pl.ds(pl.multiple_of(base_row - TILE, TILE), TILE)
            u = [grid[U, 0, r, :], grid[U, 1, r, :]]
            v = [grid[V, 0, r, :], grid[V, 1, r, :]]
            u_up = [u[1], next_row(u[0], grid[U, 0, nxt, :])]
            v_up = [v[1], next_row(v[0], grid[V, 0, nxt, :])]
            diag_xx, diag_yy, cross = [], [], []
            for y in range(2):
                sxx = east_of(u[y]) - u[y]
                syy = v_up[y] - v[y]
                shear = (u_up[y] - u[y]) + (east_of(v[y]) - v[y])
                div = sxx + syy
                ten = sxx - syy
                delta = jnp.sqrt(div * div + (ten * ten + shear * shear) * (1.0 / ECC2) + DMIN2)
                visc = RELAX * strength[y, r, :] / delta
                scale = 1.0 / (1.0 + RELAX)
                s1 = (grid[S1, y, r, :] + visc * (div - delta)) * scale
                s2 = (grid[S2, y, r, :] + visc * ten * (1.0 / ECC2)) * scale
                s12 = (grid[S12, y, r, :] + visc * shear * (0.5 / ECC2)) * scale
                grid[S1, y, r, :] = s1
                grid[S2, y, r, :] = s2
                grid[S12, y, r, :] = s12
                diag_xx.append(0.5 * (s1 + s2))
                diag_yy.append(0.5 * (s1 - s2))
                cross.append(s12)
            yy_before = 0.5 * (grid[S1, 1, prev, :] - grid[S2, 1, prev, :])
            yy_down = [last_row(diag_yy[1], yy_before), diag_yy[0]]
            cross_down = [last_row(cross[1], grid[S12, 1, prev, :]), cross[0]]
            for y in range(2):
                force_x = diag_xx[y] - west_of(diag_xx[y]) + (cross[y] - cross_down[y])
                force_y = cross[y] - west_of(cross[y]) + (diag_yy[y] - yy_down[y])
                mass = grid[MASS, y, r, :]
                act = grid[ACTIVE, y, r, :]
                cx, cy = grid[CUR_X, y, r, :], grid[CUR_Y, y, r, :]
                dx, dy = cx - u[y], cy - v[y]
                drag = dragb[y, r, :] * jnp.sqrt(dx * dx + dy * dy + DRAG_FLOOR)
                gain = act / (jnp.maximum(mass, MASS_FLOOR) * (1.0 / DTE) + drag)
                inertia = mass * (1.0 / DTE)
                turn = CORIO * mass
                grid[U, y, r, :] = gain * (
                    inertia * u[y] + force_x + grid[PUSH_X, y, r, :] + drag * cx + turn * v[y]
                )
                grid[V, y, r, :] = gain * (
                    inertia * v[y] + force_y + grid[PUSH_Y, y, r, :] + drag * cy - turn * u[y]
                )

        def sweeps(k, carry):
            sweep(k % (count // TILE + 2))
            return carry
        lax.fori_loop(0, NSUB * (count // TILE + 2), sweeps, 0)

        def returned(t, carry):
            q = pl.ds(pl.multiple_of(t * TILE, TILE), TILE)
            r = pl.ds(pl.multiple_of(first + t * TILE, TILE), TILE)
            for y in range(2):
                half = pl.ds(y * width, width)
                u, v = grid[U, y, r, main], grid[V, y, r, main]
                out[0, 0, q, half] = u
                out[0, 1, q, half] = v
                dx, dy = u - grid[CUR_X, y, r, main], v - grid[CUR_Y, y, r, main]
                drag = dragb[y, r, main] * jnp.sqrt(dx * dx + dy * dy + DRAG_FLOOR)
                forc[0, q, half] = drag * dx
                forc[1, q, half] = drag * dy
            return carry
        lax.fori_loop(0, count // TILE, returned, 0)
        for c in range(2):
            back[c] = split_dot(perm, forc[c], (1,))
        send_rows(0, back, 0, 2, ret, 0, ret_ssem.at[1], ret_rsem.at[1])
        wait_bytes(back.at[pl.ds(2, 1)], ret_ssem.at[0])
        wait_bytes(back.at[pl.ds(0, 2)], ret_ssem.at[1])


def per_device_kernel(n_lat, n_lon, fields, block_owner, ice_covered, land_mask):
    count, cells = land_mask.shape
    peers = n_lat * n_lon
    long = count + 2 * LEAD
    f32 = jnp.float32
    anywhere = pl.BlockSpec(memory_space=pl.ANY)
    in_vmem = pl.BlockSpec(memory_space=pltpu.VMEM)
    dma = pltpu.SemaphoreType.DMA
    return pl.pallas_call(
        functools.partial(step_kernel, n_lat, n_lon),
        out_shape=jax.ShapeDtypeStruct((1, 2, count, cells), f32),
        in_specs=[anywhere, in_vmem, in_vmem, anywhere],
        out_specs=in_vmem,
        scratch_shapes=[
            pltpu.VMEM((7, count, cells), f32),
            pltpu.VMEM((2, count, cells), f32),
            pltpu.VMEM((3, count, cells), f32),
            pltpu.VMEM((peers, 1, count), jnp.int32),
            pltpu.VMEM((6, count, cells), f32),
            pltpu.VMEM((12, 2, long, 2 * BX), f32),
            pltpu.VMEM((2, long, 2 * BX), f32),
            pltpu.VMEM((2, long, 2 * BX), f32),
            pltpu.VMEM((6, count, cells), f32),
            pltpu.VMEM((count, count), f32),
            pltpu.VMEM((3, count, cells), f32),
            pltpu.VMEM((count, cells), jnp.int32),
            pltpu.VMEM((2, count, BX), f32),
            pltpu.VMEM((2, count, BX), f32),
            pltpu.VMEM((2, count + 2 * TILE, BX), f32),
            pltpu.VMEM((2, count + 2 * TILE, BX), f32),
            dma((3,)), dma, dma, dma((2,)), dma((2,)), dma((2,)), dma((2,)),
            dma((8,)), dma((8,)), dma((8,)), dma((8,)),
        ],
        compiler_params=pltpu.CompilerParams(
            collective_id=0, has_side_effects=True, vmem_limit_bytes=40 * 1024 * 1024
        ),
    )(fields, block_owner.reshape(1, count), ice_covered.reshape(1, count), land_mask)


def solution(mesh):
    placed = (
        P("comp", None, ("lat", "lon"), None),
        P(("lat", "lon")),
        P(("lat", "lon")),
        P(("lat", "lon"), None),
    )
    n_lat, n_lon = mesh.shape["lat"], mesh.shape["lon"]

    def body(fields, block_owner, ice_covered, land_mask):
        count = block_owner.shape[0]
        whole_tiles = count % (n_lat * n_lon * TILE) == 0 and count == BX
        if whole_tiles and n_lon > 2:
            return per_device_kernel(n_lat, n_lon, fields, block_owner, ice_covered, land_mask)
        return per_device(fields, block_owner, ice_covered, land_mask)

    return jax.shard_map(
        body,
        mesh=mesh,
        in_specs=placed,
        out_specs=P("comp", None, ("lat", "lon"), None),
        check_vma=False,
    )
```

```python
import functools

import jax
import jax.numpy as jnp
from jax import lax
from jax.experimental import pallas as pl
from jax.experimental.pallas import tpu as pltpu
from jax.sharding import PartitionSpec as P

GX = 1
BY = 2
BX = 128
NSUB = 4


CD_ICE = 0.1
CW = 1.5
CSTAR = 2.0
ECC2 = 4.0
DMIN2 = 0.25
RELAX = 0.5
DTE = 0.5
CORIO = 0.3
MASS_FLOOR = 0.5
DRAG_FLOOR = 0.1


def from_behind(x, axis, by):
    size = lax.axis_size(axis)
    pairs = [(i, i + by) for i in range(size) if 0 <= i + by < size]
    return lax.ppermute(x, axis, pairs)


def with_halo(x, sides, width, wrap):
    for axis, dim in sides:
        size, length = (lax.axis_size(axis), x.shape[dim])
        up = [(i, (i + 1) % size) for i in range(size if wrap else size - 1)]
        down = [(j, i) for i, j in up]
        last = lax.slice_in_dim(x, length - width, length, axis=dim)
        first = lax.slice_in_dim(x, 0, width, axis=dim)
        before = lax.ppermute(last, axis, up)
        after = lax.ppermute(first, axis, down)
        x = jnp.concatenate([before, x, after], axis=dim)
    return x


def air_stress(ocean):
    wind_x, wind_y, current_x, current_y, tilt_x, tilt_y, density = ocean
    speed_ice = jnp.sqrt(wind_x * wind_x + wind_y * wind_y + 1.0)
    scale_ice = density * CD_ICE * speed_ice
    rel_x = wind_x - current_x
    rel_y = wind_y - current_y
    speed_open = jnp.sqrt(rel_x * rel_x + rel_y * rel_y + 1.0)
    scale_open = density * (0.1 + 0.05 * speed_open) * speed_open
    outbound = jnp.stack(
        [scale_ice * wind_x, scale_ice * wind_y, current_x, current_y, tilt_x, tilt_y]
    )
    open_stress = jnp.stack([scale_open * rel_x, scale_open * rel_y])
    return (outbound, open_stress)


def prepare(ice_tile, forcing, active):
    ice_mass = ice_tile[2]
    concentration = ice_tile[3]
    strength = ice_mass * jnp.exp(CSTAR * (concentration - 1.0)) * active
    drag_base = CW * concentration * active
    push_x = active * (concentration * forcing[0] - ice_mass * forcing[4])
    push_y = active * (concentration * forcing[1] - ice_mass * forcing[5])
    return jnp.stack(
        [strength, ice_mass, drag_base, push_x, push_y, forcing[2], forcing[3], active]
    )


def subcycle(ice_state, statics):
    east_vel, north_vel, stress_one, stress_two, stress_three = ice_state
    strength = statics[0]
    east_base = east_vel[:-1, :-1]
    north_base = north_vel[:-1, :-1]
    strain_xx = east_vel[:-1, 1:] - east_base
    strain_yy = north_vel[1:, :-1] - north_base
    shear = east_vel[1:, :-1] - east_base + (north_vel[:-1, 1:] - north_base)
    divergence = strain_xx + strain_yy
    tension = strain_xx - strain_yy
    delta_norm = jnp.sqrt(
        divergence * divergence + (tension * tension + shear * shear) / ECC2 + DMIN2
    )
    viscosity = strength[:-1, :-1] / delta_norm
    stress_sum = (stress_one[:-1, :-1] + RELAX * viscosity * (divergence - delta_norm)) / (
        1.0 + RELAX
    )
    stress_diff = (stress_two[:-1, :-1] + RELAX * viscosity * tension / ECC2) / (1.0 + RELAX)
    stress_shear = (stress_three[:-1, :-1] + RELAX * viscosity * shear / (2.0 * ECC2)) / (
        1.0 + RELAX
    )
    stress_xx = 0.5 * (stress_sum + stress_diff)
    stress_yy = 0.5 * (stress_sum - stress_diff)
    force_x = (
        stress_xx[1:, 1:] - stress_xx[1:, :-1] + (stress_shear[1:, 1:] - stress_shear[:-1, 1:])
    )
    force_y = (
        stress_shear[1:, 1:] - stress_shear[1:, :-1] + (stress_yy[1:, 1:] - stress_yy[:-1, 1:])
    )
    trimmed = statics[:, 1:-1, 1:-1]
    strength, ice_mass, drag_base, push_x, push_y, current_x, current_y, active = trimmed
    east_old = east_vel[1:-1, 1:-1]
    north_old = north_vel[1:-1, 1:-1]
    diff_x = current_x - east_old
    diff_y = current_y - north_old
    drag_coef = drag_base * jnp.sqrt(diff_x * diff_x + diff_y * diff_y + DRAG_FLOOR)
    denominator = jnp.maximum(ice_mass, MASS_FLOOR) / DTE + drag_coef
    east_new = (
        active
        * (
            ice_mass / DTE * east_old
            + force_x
            + push_x
            + drag_coef * current_x
            + CORIO * ice_mass * north_old
        )
        / denominator
    )
    north_new = (
        active
        * (
            ice_mass / DTE * north_old
            + force_y
            + push_y
            + drag_coef * current_y
            - CORIO * ice_mass * east_old
        )
        / denominator
    )
    new_state = jnp.stack(
        [east_new, north_new, stress_sum[1:, 1:], stress_diff[1:, 1:], stress_shear[1:, 1:]]
    )
    return (new_state, trimmed)


def give_back(ice_state, statics):
    east_vel = ice_state[0]
    north_vel = ice_state[1]
    drag_base = statics[2]
    current_x = statics[5]
    current_y = statics[6]
    diff_x = east_vel - current_x
    diff_y = north_vel - current_y
    factor = drag_base * jnp.sqrt(diff_x * diff_x + diff_y * diff_y + DRAG_FLOOR)
    return jnp.stack([factor * diff_x, factor * diff_y, drag_base / CW])


def to_tile(blocks):
    channels, count, cells = blocks.shape
    arranged = blocks.reshape(channels, count // GX, GX, BY, BX).transpose(0, 1, 3, 2, 4)
    return arranged.reshape(channels, count // GX * BY, GX * BX)


def from_tile(values):
    channels, rows, columns = values.shape
    arranged = values.reshape(channels, rows // BY, BY, GX, BX).transpose(0, 1, 3, 2, 4)
    return arranged.reshape(channels, rows // BY * GX, BY * BX)


def per_device(fields, block_owner, ice_covered, land_mask):
    count = block_owner.shape[0]
    is_ocean = lax.axis_index("comp") == 0
    outbound, open_stress = air_stress(fields[0])
    owner_row = block_owner.reshape(1, count)
    crossed = from_behind(outbound, "comp", 1)
    received, anchor = (
        lax.all_to_all(crossed, ("lat", "lon"), split_axis=1, concat_axis=1, tiled=True),
        lax.all_to_all(owner_row, ("lat", "lon"), split_axis=1, concat_axis=1, tiled=True),
    )
    local_ids = anchor[0] % count
    position = jnp.zeros((count,), jnp.int32).at[local_ids].set(jnp.arange(count, dtype=jnp.int32))
    forcing = to_tile(received[:, position])
    ice_tile = to_tile(fields[0])
    covered = ice_covered.astype(jnp.float32)[:, None] * (1 - land_mask).astype(jnp.float32)
    active = to_tile(covered[None])[0]
    statics = prepare(ice_tile, forcing, active)
    ice_state = jnp.stack([ice_tile[0], ice_tile[1], ice_tile[4], ice_tile[5], ice_tile[6]])
    joined = jnp.concatenate([ice_state, statics], 0)
    joined = with_halo(joined, (("lon", 2),), NSUB, True)
    joined = with_halo(joined, (("lat", 1),), NSUB, False)
    ice_state = joined[:5]
    statics = joined[5:]
    for repeat in range(NSUB):
        ice_state, statics = subcycle(ice_state, statics)
    returned = from_tile(give_back(ice_state, statics))
    back_send = returned[:, local_ids]
    regrouped = lax.all_to_all(back_send, ("lat", "lon"), split_axis=1, concat_axis=1, tiled=True)
    received_back = from_behind(regrouped, "comp", -1)
    ocean_out = received_back[:2] + (1.0 - received_back[2]) * open_stress
    ice_out = from_tile(ice_state[:2])
    return jnp.where(is_ocean, ocean_out, ice_out)[None]


LEAD = 16
GROUP = 3
TILE = 8
MESH = pl.DeviceIdType.MESH
DIRECTIONS = [(a, b) for a in (-1, 0, 1) for b in (-1, 0, 1) if (a, b) != (0, 0)]
U, V, MASS, CONC, S1, S2, S12, ACTIVE, PUSH_X, PUSH_Y, CUR_X, CUR_Y = range(12)


def tile_loop(tiles, together, body):
    def step(k, carry):
        for j in range(together):
            body(k * together + j)
        return carry
    lax.fori_loop(0, tiles // together, step, 0)


def split_dot(one_hot, values, contract):
    total = None
    rest = values
    for piece in range(3):
        part = rest.astype(jnp.bfloat16)
        if piece < 2:
            rest = rest - part.astype(jnp.float32)
        term = lax.dot_general(
            one_hot, part, ((contract, (0,)), ((), ())), preferred_element_type=jnp.float32
        )
        total = term if total is None else total + term
    return total


def step_kernel(
    n_lat, n_lon,
    fields, owner, covered, land, out,
    surf, open_st, ret, ids, recv, grid, strength, dragb, forc, one_hot, back, land_v,
    pack_early, pack_mid, pack_late, got_early, got_mid, got_late,
    load_sem, ids_ssem, ids_rsem, fwd_ssem, fwd_rsem, ret_ssem, ret_rsem,
    early_ssem, early_rsem, mid_ssem, mid_rsem, late_ssem, late_rsem,
):
    comp = lax.axis_index("comp")
    lat = lax.axis_index("lat")
    lon = lax.axis_index("lon")
    peers = n_lat * n_lon
    me = lat * n_lon + lon
    count = owner.shape[1]
    per = count // peers
    width = BX
    barrier = pltpu.get_barrier_semaphore()

    def rows_of(peer):
        return pl.ds(pl.multiple_of(peer * per, per), per)

    def device(kind, peer):
        return (kind, peer // n_lon, peer % n_lon)

    def each_peer(body):
        def step(k, carry):
            body((me + peers // 2 + k) % peers)
            return carry
        lax.fori_loop(0, peers, step, 0)

    def signal_peers(kind):
        each_peer(
            lambda p: pl.semaphore_signal(
                barrier, inc=1, device_id=device(kind, p), device_id_type=MESH
            )
        )

    def send_rows(kind, src, lo, num, dst, dlo, ssem, rsem):
        def body(p):
            pltpu.make_async_remote_copy(
                src_ref=src.at[pl.ds(lo, num), rows_of(p), :],
                dst_ref=dst.at[pl.ds(dlo, num), rows_of(me), :],
                send_sem=ssem, recv_sem=rsem,
                device_id=device(kind, p), device_id_type=MESH,
            ).start()
        each_peer(body)

    def wait_bytes(ref, sem):
        pltpu.make_async_copy(ref, ref, sem).wait()

    @pl.when(comp == 0)
    def _ocean():
        raw = pltpu.make_async_copy(fields.at[0, pl.ds(2, 4)], surf.at[pl.ds(2, 4)], load_sem.at[0])
        wind = pltpu.make_async_copy(fields.at[0, pl.ds(0, 2)], surf.at[pl.ds(0, 2)], load_sem.at[1])
        rho = pltpu.make_async_copy(fields.at[0, pl.ds(6, 1)], surf.at[pl.ds(6, 1)], load_sem.at[2])
        raw.start()
        wind.start()
        rho.start()
        signal_peers(1)
        pl.semaphore_wait(barrier, peers)

        def ids_out(p):
            pltpu.make_async_remote_copy(
                src_ref=owner, dst_ref=ids.at[me], send_sem=ids_ssem, recv_sem=ids_rsem,
                device_id=device(1, p), device_id_type=MESH,
            ).start()
        each_peer(ids_out)
        raw.wait()
        send_rows(1, surf, 2, 4, recv, 2, fwd_ssem.at[0], fwd_rsem.at[0])
        wind.wait()
        rho.wait()

        def stress(t):
            r = pl.ds(pl.multiple_of(t * TILE, TILE), TILE)
            wx, wy, density = surf[0, r, :], surf[1, r, :], surf[6, r, :]
            scale = density * CD_ICE * jnp.sqrt(wx * wx + wy * wy + 1.0)
            forc[0, r, :] = scale * wx
            forc[1, r, :] = scale * wy

        tile_loop(count // TILE, 2, stress)
        send_rows(1, forc, 0, 2, recv, 0, fwd_ssem.at[1], fwd_rsem.at[1])

        def open_water(t):
            r = pl.ds(pl.multiple_of(t * TILE, TILE), TILE)
            density = surf[6, r, :]
            rel_x = surf[0, r, :] - surf[2, r, :]
            rel_y = surf[1, r, :] - surf[3, r, :]
            speed = jnp.sqrt(rel_x * rel_x + rel_y * rel_y + 1.0)
            scale = density * (0.1 + 0.05 * speed) * speed
            open_st[0, r, :] = scale * rel_x
            open_st[1, r, :] = scale * rel_y

        tile_loop(count // TILE, 2, open_water)
        wait_bytes(ret.at[pl.ds(2, 1)], ret_rsem.at[0])
        wait_bytes(ret.at[pl.ds(0, 2)], ret_rsem.at[1])

        def finish(t):
            r = pl.ds(pl.multiple_of(t * TILE, TILE), TILE)
            water = 1.0 - ret[2, r, :]
            out[0, 0, r, :] = ret[0, r, :] + water * open_st[0, r, :]
            out[0, 1, r, :] = ret[1, r, :] + water * open_st[1, r, :]

        tile_loop(count // TILE, 2, finish)
        wait_bytes(ids, ids_ssem)
        wait_bytes(surf.at[pl.ds(2, 4)], fwd_ssem.at[0])
        wait_bytes(forc.at[pl.ds(0, 2)], fwd_ssem.at[1])

    @pl.when(comp == 1)
    def _ice():
        first, last = LEAD, LEAD + count
        core = pl.ds(first, count)
        main, side = pl.ds(0, width), pl.ds(width, width)
        loads = [
            pltpu.make_async_copy(
                fields.at[0, :, :, pl.ds(y * width, width)],
                grid.at[pl.ds(0, 7), y, core, main],
                load_sem.at[y],
            )
            for y in range(2)
        ]
        loads.append(pltpu.make_async_copy(land, land_v, load_sem.at[2]))
        for load in loads:
            load.start()
        for c in range(12):
            for y in range(2):
                blank = jnp.zeros((LEAD, 2 * width), jnp.float32)
                grid[c, y, pl.ds(0, LEAD), :] = blank
                grid[c, y, pl.ds(last, LEAD), :] = blank
        for got in (got_early, got_mid, got_late):
            for d in range(2):
                got[d, pl.ds(0, TILE), :] = jnp.zeros((TILE, width), jnp.float32)
                got[d, pl.ds(TILE + count, TILE), :] = jnp.zeros((TILE, width), jnp.float32)

        def inside(a):
            if a == 0:
                return lat >= 0
            return lat + a >= 0 if a < 0 else lat + a < n_lat

        signal_peers(0)
        for a, b in DIRECTIONS:
            @pl.when(inside(a))
            def _():
                pl.semaphore_signal(
                    barrier, inc=1, device_id=(1, lat + a, (lon + b + n_lon) % n_lon),
                    device_id_type=MESH,
                )
        walls = jnp.where(lat == 0, 3, 0) + jnp.where(lat == n_lat - 1, 3, 0)
        pl.semaphore_wait(barrier, peers + 8 - walls)
        for load in loads:
            load.wait()

        diag = lax.broadcasted_iota(jnp.int32, (count, count), 0) == lax.broadcasted_iota(
            jnp.int32, (count, count), 1
        )
        wet = jnp.sum(
            jnp.where(diag, covered[...].astype(jnp.float32), 0.0), axis=1, keepdims=True
        )
        sea = wet * (1 - land_v[...]).astype(jnp.float32)
        for y in range(2):
            grid[ACTIVE, y, core, main] = sea[:, y * width:(y + 1) * width]

        lane = lax.broadcasted_iota(jnp.int32, (TILE, width), 1)

        def pack(lo, num, packed):
            def body(t):
                r = pl.ds(pl.multiple_of(first + t * TILE, TILE), TILE)
                east = jnp.zeros((TILE, width), jnp.float32)
                west = east
                for c in range(num):
                    for y in range(2):
                        x = grid[lo + c, y, r, main]
                        slot = (c * 2 + y) * NSUB
                        mine = (lane >= slot) & (lane < slot + NSUB)
                        east = jnp.where(mine, pltpu.roll(x, (slot + NSUB) % width, 1), east)
                        west = jnp.where(mine, pltpu.roll(x, slot, 1) if slot else x, west)
                q = pl.ds(pl.multiple_of(t * TILE, TILE), TILE)
                packed[0, q, :] = east
                packed[1, q, :] = west
            tile_loop(count // TILE, 2, body)

        def halo(lo, num, packed, got, ssem, rsem, begin):
            for k, (a, b) in enumerate(DIRECTIONS):
                src_row = {-1: 0, 0: 0, 1: count - TILE}[a]
                dst_row = {-1: count, 0: 0, 1: -TILE}[a]
                rows = count if a == 0 else TILE
                if b == 0:
                    src = grid.at[pl.ds(lo, num), :, pl.ds(first + src_row, rows), main]
                    dst = grid.at[pl.ds(lo, num), :, pl.ds(first + dst_row, rows), main]
                else:
                    d = 0 if b > 0 else 1
                    src = packed.at[d, pl.ds(src_row, rows), :]
                    dst = got.at[d, pl.ds(TILE + dst_row, rows), :]
                copy = pltpu.make_async_remote_copy(
                    src_ref=src, dst_ref=dst, send_sem=ssem.at[k], recv_sem=rsem.at[k],
                    device_id=(1, lat + a, (lon + b + n_lon) % n_lon), device_id_type=MESH,
                )
                if begin:
                    @pl.when(inside(a))
                    def _():
                        copy.start()
                else:
                    @pl.when(inside(a))
                    def _():
                        copy.wait_send()

                    @pl.when(inside(-a))
                    def _():
                        copy.wait_recv()

        def side_of(got, slot, q):
            east = got[1, q, :]
            west = got[0, q, :]
            east = pltpu.roll(east, (width - slot) % width, 1) if slot else east
            west = pltpu.roll(west, width - NSUB - slot, 1)
            return jnp.where(
                lane < NSUB, east, jnp.where(lane >= width - NSUB, west, 0.0)
            )

        def unpack(lo, num, got, after):
            def body(t):
                q = pl.ds(pl.multiple_of(t * TILE, TILE), TILE)
                r = pl.ds(pl.multiple_of(first + (t - 1) * TILE, TILE), TILE)
                for c in range(num):
                    for y in range(2):
                        grid[lo + c, y, r, side] = side_of(got, (c * 2 + y) * NSUB, q)
                after(r)
            tile_loop(count // TILE + 2, 2, body)

        pack(0, 8, pack_early)
        halo(0, 8, pack_early, got_early, early_ssem, early_rsem, True)

        def ice_statics(r):
            for y in range(2):
                conc = grid[CONC, y, r, :]
                act = grid[ACTIVE, y, r, :]
                strength[y, r, :] = (
                    (RELAX / (1.0 + RELAX)) * grid[MASS, y, r, :] * jnp.exp(CSTAR * (conc - 1.0)) * act
                )
                dragb[y, r, :] = CW * conc * act

        wait_bytes(ids, ids_rsem)
        wanted = me * per
        row_lane = lax.broadcasted_iota(jnp.int32, (per, count), 1)
        row_sub = lax.broadcasted_iota(jnp.int32, (per, count), 0)
        mine = row_lane == row_sub + wanted
        blocks = lax.broadcasted_iota(jnp.int32, (per, count), 1).astype(jnp.float32)
        base = (me * count).astype(jnp.float32)
        for p in range(peers):
            owned = jnp.broadcast_to(ids[p], (per, count)).astype(jnp.float32)
            local = jnp.sum(jnp.where(mine, owned, 0.0), axis=1, keepdims=True) - base
            one_hot[pl.ds(p * per, per), :] = jnp.where(local == blocks, 1.0, 0.0)

        halo(0, 8, pack_early, got_early, early_ssem, early_rsem, False)
        unpack(0, 8, got_early, ice_statics)

        def east_of(x):
            return pltpu.roll(x, 2 * width - 1, 1)

        def west_of(x):
            return pltpu.roll(x, 1, 1)

        sub = lax.broadcasted_iota(jnp.int32, (TILE, 2 * width), 0)

        def next_row(x, after):
            return pltpu.roll(jnp.where(sub == 0, after, x), TILE - 1, 0)

        def last_row(x, before):
            return pltpu.roll(jnp.where(sub == TILE - 1, before, x), 1, 0)

        def sweep(g, new_stress, new_velocity):
            spots = [
                pl.ds(pl.multiple_of(first + (g * GROUP + j - 2) * TILE, TILE), TILE)
                for j in range(GROUP + 2)
            ]
            before, spots, after = spots[0], spots[1:-1], spots[-1]
            keep = 1.0 / (1.0 + RELAX)
            vels, stresses = [], []
            for r in spots:
                vels.append([(grid[U, y, r, :], grid[V, y, r, :]) for y in range(2)])
            if new_stress:
                follow = (grid[U, 0, after, :], grid[V, 0, after, :])
            for j, r in enumerate(spots):
                if not new_stress:
                    stresses.append(
                        [tuple(grid[c, y, r, :] for c in (S1, S2, S12)) for y in range(2)]
                    )
                    continue
                beyond = vels[j + 1][0] if j + 1 < GROUP else follow
                row = []
                for y in range(2):
                    u, v = vels[j][y]
                    if y == 0:
                        u_up, v_up = vels[j][1]
                    else:
                        u_up = next_row(vels[j][0][0], beyond[0])
                        v_up = next_row(vels[j][0][1], beyond[1])
                    sxx = east_of(u) - u
                    syy = v_up - v
                    shear = (u_up - u) + (east_of(v) - v)
                    div = sxx + syy
                    ten = sxx - syy
                    square = div * div + (ten * ten + shear * shear) * (1.0 / ECC2) + DMIN2
                    inverse = lax.rsqrt(square)
                    visc = strength[y, r, :] * inverse
                    s1 = grid[S1, y, r, :] * keep + visc * (div - square * inverse)
                    s2 = grid[S2, y, r, :] * keep + visc * ten * (1.0 / ECC2)
                    s12 = grid[S12, y, r, :] * keep + visc * shear * (0.5 / ECC2)
                    grid[S1, y, r, :] = s1
                    grid[S2, y, r, :] = s2
                    grid[S12, y, r, :] = s12
                    row.append((s1, s2, s12))
                stresses.append(row)
            if not new_velocity:
                return
            yy_before = 0.5 * (grid[S1, 1, before, :] - grid[S2, 1, before, :])
            cross_before = grid[S12, 1, before, :]
            for j, r in enumerate(spots):
                xx = [0.5 * (s1 + s2) for s1, s2, _ in stresses[j]]
                yy = [0.5 * (s1 - s2) for s1, s2, _ in stresses[j]]
                cross = [s12 for _, _, s12 in stresses[j]]
                yy_down = [last_row(yy[1], yy_before), yy[0]]
                cross_down = [last_row(cross[1], cross_before), cross[0]]
                yy_before, cross_before = yy[1], cross[1]
                for y in range(2):
                    u, v = vels[j][y]
                    force_x = xx[y] - west_of(xx[y]) + (cross[y] - cross_down[y])
                    force_y = cross[y] - west_of(cross[y]) + (yy[y] - yy_down[y])
                    mass = grid[MASS, y, r, :]
                    cx, cy = grid[CUR_X, y, r, :], grid[CUR_Y, y, r, :]
                    dx, dy = cx - u, cy - v
                    square = dx * dx + dy * dy + DRAG_FLOOR
                    drag = dragb[y, r, :] * (square * lax.rsqrt(square))
                    gain = grid[ACTIVE, y, r, :] / (
                        jnp.maximum(mass, MASS_FLOOR) * (1.0 / DTE) + drag
                    )
                    inertia = mass * (1.0 / DTE)
                    turn = CORIO * mass
                    grid[U, y, r, :] = gain * (
                        inertia * u + force_x + grid[PUSH_X, y, r, :] + drag * cx + turn * v
                    )
                    grid[V, y, r, :] = gain * (
                        inertia * v + force_y + grid[PUSH_Y, y, r, :] + drag * cy - turn * u
                    )

        groups = (count // TILE + 2) // GROUP

        def stress_only():
            tile_loop(groups, 1, lambda g: sweep(g, True, False))

        perm = one_hot[...].astype(jnp.bfloat16)
        stress_only()
        wait_bytes(recv.at[pl.ds(2, 4)], fwd_rsem.at[0])
        for c in range(2):
            both = split_dot(perm, recv[2 + c], (0,))
            for y in range(2):
                grid[CUR_X + c, y, core, main] = both[:, y * width:(y + 1) * width]
        pack(CUR_X, 2, pack_mid)
        halo(CUR_X, 2, pack_mid, got_mid, mid_ssem, mid_rsem, True)
        for c in range(2):
            both = split_dot(perm, recv[4 + c], (0,))
            for y in range(2):
                part = both[:, y * width:(y + 1) * width]
                grid[PUSH_X + c, y, core, main] = grid[MASS, y, core, main] * part
        halo(CUR_X, 2, pack_mid, got_mid, mid_ssem, mid_rsem, False)
        unpack(CUR_X, 2, got_mid, lambda r: None)
        wait_bytes(recv.at[pl.ds(0, 2)], fwd_rsem.at[1])
        for c in range(2):
            both = split_dot(perm, recv[c], (0,))
            for y in range(2):
                part = both[:, y * width:(y + 1) * width]
                grid[PUSH_X + c, y, core, main] = grid[ACTIVE, y, core, main] * (
                    grid[CONC, y, core, main] * part - grid[PUSH_X + c, y, core, main]
                )
        pack(PUSH_X, 2, pack_late)
        halo(PUSH_X, 2, pack_late, got_late, late_ssem, late_rsem, True)

        for y in range(2):
            share = grid[CONC, y, core, main] * grid[ACTIVE, y, core, main]
            back[2, :, pl.ds(y * width, width)] = split_dot(perm, share, (1,))
        send_rows(0, back, 2, 1, ret, 2, ret_ssem.at[0], ret_rsem.at[0])

        halo(PUSH_X, 2, pack_late, got_late, late_ssem, late_rsem, False)
        unpack(PUSH_X, 2, got_late, lambda r: None)
        tile_loop(groups, 1, lambda g: sweep(g, False, True))
        tile_loop((NSUB - 1) * groups, 1, lambda k: sweep(k % groups, True, True))

        def returned(t):
            q = pl.ds(pl.multiple_of(t * TILE, TILE), TILE)
            r = pl.ds(pl.multiple_of(first + t * TILE, TILE), TILE)
            for y in range(2):
                half = pl.ds(y * width, width)
                u, v = grid[U, y, r, main], grid[V, y, r, main]
                out[0, 0, q, half] = u
                out[0, 1, q, half] = v
                dx, dy = u - grid[CUR_X, y, r, main], v - grid[CUR_Y, y, r, main]
                drag = dragb[y, r, main] * jnp.sqrt(dx * dx + dy * dy + DRAG_FLOOR)
                forc[0, q, half] = drag * dx
                forc[1, q, half] = drag * dy

        tile_loop(count // TILE, 2, returned)
        for c in range(2):
            back[c] = split_dot(perm, forc[c], (1,))
        send_rows(0, back, 0, 2, ret, 0, ret_ssem.at[1], ret_rsem.at[1])
        wait_bytes(back.at[pl.ds(2, 1)], ret_ssem.at[0])
        wait_bytes(back.at[pl.ds(0, 2)], ret_ssem.at[1])


def per_device_kernel(n_lat, n_lon, fields, block_owner, ice_covered, land_mask):
    count, cells = land_mask.shape
    peers = n_lat * n_lon
    long = count + 2 * LEAD
    f32 = jnp.float32
    anywhere = pl.BlockSpec(memory_space=pl.ANY)
    in_vmem = pl.BlockSpec(memory_space=pltpu.VMEM)
    dma = pltpu.SemaphoreType.DMA
    return pl.pallas_call(
        functools.partial(step_kernel, n_lat, n_lon),
        out_shape=jax.ShapeDtypeStruct((1, 2, count, cells), f32),
        in_specs=[anywhere, in_vmem, in_vmem, anywhere],
        out_specs=in_vmem,
        scratch_shapes=[
            pltpu.VMEM((7, count, cells), f32),
            pltpu.VMEM((2, count, cells), f32),
            pltpu.VMEM((3, count, cells), f32),
            pltpu.VMEM((peers, 1, count), jnp.int32),
            pltpu.VMEM((6, count, cells), f32),
            pltpu.VMEM((12, 2, long, 2 * BX), f32),
            pltpu.VMEM((2, long, 2 * BX), f32),
            pltpu.VMEM((2, long, 2 * BX), f32),
            pltpu.VMEM((6, count, cells), f32),
            pltpu.VMEM((count, count), f32),
            pltpu.VMEM((3, count, cells), f32),
            pltpu.VMEM((count, cells), jnp.int32),
            pltpu.VMEM((2, count, BX), f32),
            pltpu.VMEM((2, count, BX), f32),
            pltpu.VMEM((2, count, BX), f32),
            pltpu.VMEM((2, count + 2 * TILE, BX), f32),
            pltpu.VMEM((2, count + 2 * TILE, BX), f32),
            pltpu.VMEM((2, count + 2 * TILE, BX), f32),
            dma((3,)), dma, dma, dma((2,)), dma((2,)), dma((2,)), dma((2,)),
            dma((8,)), dma((8,)), dma((8,)), dma((8,)), dma((8,)), dma((8,)),
        ],
        compiler_params=pltpu.CompilerParams(
            collective_id=0, has_side_effects=True, vmem_limit_bytes=63 * 1024 * 1024
        ),
    )(fields, block_owner.reshape(1, count), ice_covered.reshape(1, count), land_mask)


def solution(mesh):
    placed = (
        P("comp", None, ("lat", "lon"), None),
        P(("lat", "lon")),
        P(("lat", "lon")),
        P(("lat", "lon"), None),
    )
    n_lat, n_lon = mesh.shape["lat"], mesh.shape["lon"]

    def body(fields, block_owner, ice_covered, land_mask):
        count = block_owner.shape[0]
        whole_tiles = count % (n_lat * n_lon * TILE) == 0 and count == BX
        if whole_tiles and n_lon > 2:
            return per_device_kernel(n_lat, n_lon, fields, block_owner, ice_covered, land_mask)
        return per_device(fields, block_owner, ice_covered, land_mask)

    return jax.shard_map(
        body,
        mesh=mesh,
        in_specs=placed,
        out_specs=P("comp", None, ("lat", "lon"), None),
        check_vma=False,
    )
```

```python
import functools

import jax
import jax.numpy as jnp
from jax import lax
from jax.experimental import pallas as pl
from jax.experimental.pallas import tpu as pltpu
from jax.sharding import PartitionSpec as P

GX = 1
BY = 2
BX = 128
NSUB = 4


CD_ICE = 0.1
CW = 1.5
CSTAR = 2.0
ECC2 = 4.0
DMIN2 = 0.25
RELAX = 0.5
DTE = 0.5
CORIO = 0.3
MASS_FLOOR = 0.5
DRAG_FLOOR = 0.1


def from_behind(x, axis, by):
    size = lax.axis_size(axis)
    pairs = [(i, i + by) for i in range(size) if 0 <= i + by < size]
    return lax.ppermute(x, axis, pairs)


def with_halo(x, sides, width, wrap):
    for axis, dim in sides:
        size, length = (lax.axis_size(axis), x.shape[dim])
        up = [(i, (i + 1) % size) for i in range(size if wrap else size - 1)]
        down = [(j, i) for i, j in up]
        last = lax.slice_in_dim(x, length - width, length, axis=dim)
        first = lax.slice_in_dim(x, 0, width, axis=dim)
        before = lax.ppermute(last, axis, up)
        after = lax.ppermute(first, axis, down)
        x = jnp.concatenate([before, x, after], axis=dim)
    return x


def air_stress(ocean):
    wind_x, wind_y, current_x, current_y, tilt_x, tilt_y, density = ocean
    speed_ice = jnp.sqrt(wind_x * wind_x + wind_y * wind_y + 1.0)
    scale_ice = density * CD_ICE * speed_ice
    rel_x = wind_x - current_x
    rel_y = wind_y - current_y
    speed_open = jnp.sqrt(rel_x * rel_x + rel_y * rel_y + 1.0)
    scale_open = density * (0.1 + 0.05 * speed_open) * speed_open
    outbound = jnp.stack(
        [scale_ice * wind_x, scale_ice * wind_y, current_x, current_y, tilt_x, tilt_y]
    )
    open_stress = jnp.stack([scale_open * rel_x, scale_open * rel_y])
    return (outbound, open_stress)


def prepare(ice_tile, forcing, active):
    ice_mass = ice_tile[2]
    concentration = ice_tile[3]
    strength = ice_mass * jnp.exp(CSTAR * (concentration - 1.0)) * active
    drag_base = CW * concentration * active
    push_x = active * (concentration * forcing[0] - ice_mass * forcing[4])
    push_y = active * (concentration * forcing[1] - ice_mass * forcing[5])
    return jnp.stack(
        [strength, ice_mass, drag_base, push_x, push_y, forcing[2], forcing[3], active]
    )


def subcycle(ice_state, statics):
    east_vel, north_vel, stress_one, stress_two, stress_three = ice_state
    strength = statics[0]
    east_base = east_vel[:-1, :-1]
    north_base = north_vel[:-1, :-1]
    strain_xx = east_vel[:-1, 1:] - east_base
    strain_yy = north_vel[1:, :-1] - north_base
    shear = east_vel[1:, :-1] - east_base + (north_vel[:-1, 1:] - north_base)
    divergence = strain_xx + strain_yy
    tension = strain_xx - strain_yy
    delta_norm = jnp.sqrt(
        divergence * divergence + (tension * tension + shear * shear) / ECC2 + DMIN2
    )
    viscosity = strength[:-1, :-1] / delta_norm
    stress_sum = (stress_one[:-1, :-1] + RELAX * viscosity * (divergence - delta_norm)) / (
        1.0 + RELAX
    )
    stress_diff = (stress_two[:-1, :-1] + RELAX * viscosity * tension / ECC2) / (1.0 + RELAX)
    stress_shear = (stress_three[:-1, :-1] + RELAX * viscosity * shear / (2.0 * ECC2)) / (
        1.0 + RELAX
    )
    stress_xx = 0.5 * (stress_sum + stress_diff)
    stress_yy = 0.5 * (stress_sum - stress_diff)
    force_x = (
        stress_xx[1:, 1:] - stress_xx[1:, :-1] + (stress_shear[1:, 1:] - stress_shear[:-1, 1:])
    )
    force_y = (
        stress_shear[1:, 1:] - stress_shear[1:, :-1] + (stress_yy[1:, 1:] - stress_yy[:-1, 1:])
    )
    trimmed = statics[:, 1:-1, 1:-1]
    strength, ice_mass, drag_base, push_x, push_y, current_x, current_y, active = trimmed
    east_old = east_vel[1:-1, 1:-1]
    north_old = north_vel[1:-1, 1:-1]
    diff_x = current_x - east_old
    diff_y = current_y - north_old
    drag_coef = drag_base * jnp.sqrt(diff_x * diff_x + diff_y * diff_y + DRAG_FLOOR)
    denominator = jnp.maximum(ice_mass, MASS_FLOOR) / DTE + drag_coef
    east_new = (
        active
        * (
            ice_mass / DTE * east_old
            + force_x
            + push_x
            + drag_coef * current_x
            + CORIO * ice_mass * north_old
        )
        / denominator
    )
    north_new = (
        active
        * (
            ice_mass / DTE * north_old
            + force_y
            + push_y
            + drag_coef * current_y
            - CORIO * ice_mass * east_old
        )
        / denominator
    )
    new_state = jnp.stack(
        [east_new, north_new, stress_sum[1:, 1:], stress_diff[1:, 1:], stress_shear[1:, 1:]]
    )
    return (new_state, trimmed)


def give_back(ice_state, statics):
    east_vel = ice_state[0]
    north_vel = ice_state[1]
    drag_base = statics[2]
    current_x = statics[5]
    current_y = statics[6]
    diff_x = east_vel - current_x
    diff_y = north_vel - current_y
    factor = drag_base * jnp.sqrt(diff_x * diff_x + diff_y * diff_y + DRAG_FLOOR)
    return jnp.stack([factor * diff_x, factor * diff_y, drag_base / CW])


def to_tile(blocks):
    channels, count, cells = blocks.shape
    arranged = blocks.reshape(channels, count // GX, GX, BY, BX).transpose(0, 1, 3, 2, 4)
    return arranged.reshape(channels, count // GX * BY, GX * BX)


def from_tile(values):
    channels, rows, columns = values.shape
    arranged = values.reshape(channels, rows // BY, BY, GX, BX).transpose(0, 1, 3, 2, 4)
    return arranged.reshape(channels, rows // BY * GX, BY * BX)


def per_device(fields, block_owner, ice_covered, land_mask):
    count = block_owner.shape[0]
    is_ocean = lax.axis_index("comp") == 0
    outbound, open_stress = air_stress(fields[0])
    owner_row = block_owner.reshape(1, count)
    crossed = from_behind(outbound, "comp", 1)
    received, anchor = (
        lax.all_to_all(crossed, ("lat", "lon"), split_axis=1, concat_axis=1, tiled=True),
        lax.all_to_all(owner_row, ("lat", "lon"), split_axis=1, concat_axis=1, tiled=True),
    )
    local_ids = anchor[0] % count
    position = jnp.zeros((count,), jnp.int32).at[local_ids].set(jnp.arange(count, dtype=jnp.int32))
    forcing = to_tile(received[:, position])
    ice_tile = to_tile(fields[0])
    covered = ice_covered.astype(jnp.float32)[:, None] * (1 - land_mask).astype(jnp.float32)
    active = to_tile(covered[None])[0]
    statics = prepare(ice_tile, forcing, active)
    ice_state = jnp.stack([ice_tile[0], ice_tile[1], ice_tile[4], ice_tile[5], ice_tile[6]])
    joined = jnp.concatenate([ice_state, statics], 0)
    joined = with_halo(joined, (("lon", 2),), NSUB, True)
    joined = with_halo(joined, (("lat", 1),), NSUB, False)
    ice_state = joined[:5]
    statics = joined[5:]
    for repeat in range(NSUB):
        ice_state, statics = subcycle(ice_state, statics)
    returned = from_tile(give_back(ice_state, statics))
    back_send = returned[:, local_ids]
    regrouped = lax.all_to_all(back_send, ("lat", "lon"), split_axis=1, concat_axis=1, tiled=True)
    received_back = from_behind(regrouped, "comp", -1)
    ocean_out = received_back[:2] + (1.0 - received_back[2]) * open_stress
    ice_out = from_tile(ice_state[:2])
    return jnp.where(is_ocean, ocean_out, ice_out)[None]


LEAD = 16
GROUP = 6
TILE = 8
MESH = pl.DeviceIdType.MESH
DIRECTIONS = [(a, b) for a in (-1, 0, 1) for b in (-1, 0, 1) if (a, b) != (0, 0)]
U, V, MASS, CONC, S1, S2, S12, ACTIVE, PUSH_X, PUSH_Y, CUR_X, CUR_Y = range(12)


def tile_loop(tiles, together, body):
    def step(k, carry):
        for j in range(together):
            body(k * together + j)
        return carry
    lax.fori_loop(0, tiles // together, step, 0)


def split_dot(one_hot, values, contract):
    total = None
    rest = values
    for piece in range(3):
        part = rest.astype(jnp.bfloat16)
        if piece < 2:
            rest = rest - part.astype(jnp.float32)
        term = lax.dot_general(
            one_hot, part, ((contract, (0,)), ((), ())), preferred_element_type=jnp.float32
        )
        total = term if total is None else total + term
    return total


def step_kernel(
    n_lat, n_lon,
    fields, owner, covered, land, out,
    surf, open_st, ret, ids, recv, grid, strength, dragb, forc, one_hot, back, land_v,
    pack_early, pack_mid, pack_late, got_early, got_mid, got_late,
    load_sem, ids_ssem, ids_rsem, fwd_ssem, fwd_rsem, ret_ssem, ret_rsem,
    early_ssem, early_rsem, mid_ssem, mid_rsem, late_ssem, late_rsem,
):
    comp = lax.axis_index("comp")
    lat = lax.axis_index("lat")
    lon = lax.axis_index("lon")
    peers = n_lat * n_lon
    me = lat * n_lon + lon
    count = owner.shape[1]
    per = count // peers
    width = BX
    barrier = pltpu.get_barrier_semaphore()

    def rows_of(peer):
        return pl.ds(pl.multiple_of(peer * per, per), per)

    def device(kind, peer):
        return (kind, peer // n_lon, peer % n_lon)

    def each_peer(body):
        def step(k, carry):
            body((me + k) % peers)
            return carry
        lax.fori_loop(0, peers, step, 0)

    def signal_peers(kind):
        each_peer(
            lambda p: pl.semaphore_signal(
                barrier, inc=1, device_id=device(kind, p), device_id_type=MESH
            )
        )

    def send_rows(kind, src, lo, num, dst, dlo, ssem, rsem):
        def body(p):
            pltpu.make_async_remote_copy(
                src_ref=src.at[pl.ds(lo, num), rows_of(p), :],
                dst_ref=dst.at[pl.ds(dlo, num), rows_of(me), :],
                send_sem=ssem, recv_sem=rsem,
                device_id=device(kind, p), device_id_type=MESH,
            ).start()
        each_peer(body)

    def wait_bytes(ref, sem):
        pltpu.make_async_copy(ref, ref, sem).wait()

    @pl.when(comp == 0)
    def _ocean():
        raw = pltpu.make_async_copy(fields.at[0, pl.ds(2, 4)], surf.at[pl.ds(2, 4)], load_sem.at[0])
        wind = pltpu.make_async_copy(fields.at[0, pl.ds(0, 2)], surf.at[pl.ds(0, 2)], load_sem.at[1])
        rho = pltpu.make_async_copy(fields.at[0, pl.ds(6, 1)], surf.at[pl.ds(6, 1)], load_sem.at[2])
        raw.start()
        wind.start()
        rho.start()
        signal_peers(1)
        pl.semaphore_wait(barrier, peers)

        def ids_out(p):
            pltpu.make_async_remote_copy(
                src_ref=owner, dst_ref=ids.at[me], send_sem=ids_ssem, recv_sem=ids_rsem,
                device_id=device(1, p), device_id_type=MESH,
            ).start()
        each_peer(ids_out)
        raw.wait()
        send_rows(1, surf, 2, 4, recv, 2, fwd_ssem.at[0], fwd_rsem.at[0])
        wind.wait()
        rho.wait()

        def stress(t):
            r = pl.ds(pl.multiple_of(t * TILE, TILE), TILE)
            wx, wy, density = surf[0, r, :], surf[1, r, :], surf[6, r, :]
            scale = density * CD_ICE * jnp.sqrt(wx * wx + wy * wy + 1.0)
            forc[0, r, :] = scale * wx
            forc[1, r, :] = scale * wy

        tile_loop(count // TILE, 2, stress)
        send_rows(1, forc, 0, 2, recv, 0, fwd_ssem.at[1], fwd_rsem.at[1])

        def open_water(t):
            r = pl.ds(pl.multiple_of(t * TILE, TILE), TILE)
            density = surf[6, r, :]
            rel_x = surf[0, r, :] - surf[2, r, :]
            rel_y = surf[1, r, :] - surf[3, r, :]
            speed = jnp.sqrt(rel_x * rel_x + rel_y * rel_y + 1.0)
            scale = density * (0.1 + 0.05 * speed) * speed
            open_st[0, r, :] = scale * rel_x
            open_st[1, r, :] = scale * rel_y

        tile_loop(count // TILE, 2, open_water)
        wait_bytes(ret.at[pl.ds(2, 1)], ret_rsem.at[0])
        wait_bytes(ret.at[pl.ds(0, 2)], ret_rsem.at[1])

        def finish(t):
            r = pl.ds(pl.multiple_of(t * TILE, TILE), TILE)
            water = 1.0 - ret[2, r, :]
            out[0, 0, r, :] = ret[0, r, :] + water * open_st[0, r, :]
            out[0, 1, r, :] = ret[1, r, :] + water * open_st[1, r, :]

        tile_loop(count // TILE, 2, finish)
        wait_bytes(ids, ids_ssem)
        wait_bytes(surf.at[pl.ds(2, 4)], fwd_ssem.at[0])
        wait_bytes(forc.at[pl.ds(0, 2)], fwd_ssem.at[1])

    @pl.when(comp == 1)
    def _ice():
        first, last = LEAD, LEAD + count
        core = pl.ds(first, count)
        main, side = pl.ds(0, width), pl.ds(width, width)
        loads = [
            pltpu.make_async_copy(
                fields.at[0, :, :, pl.ds(y * width, width)],
                grid.at[pl.ds(0, 7), y, core, main],
                load_sem.at[y],
            )
            for y in range(2)
        ]
        loads.append(pltpu.make_async_copy(land, land_v, load_sem.at[2]))
        for load in loads:
            load.start()
        for c in range(12):
            for y in range(2):
                blank = jnp.zeros((LEAD, 2 * width), jnp.float32)
                grid[c, y, pl.ds(0, LEAD), :] = blank
                grid[c, y, pl.ds(last, LEAD), :] = blank
        for got in (got_early, got_mid, got_late):
            for d in range(2):
                got[d, pl.ds(0, TILE), :] = jnp.zeros((TILE, width), jnp.float32)
                got[d, pl.ds(TILE + count, TILE), :] = jnp.zeros((TILE, width), jnp.float32)

        def inside(a):
            if a == 0:
                return lat >= 0
            return lat + a >= 0 if a < 0 else lat + a < n_lat

        signal_peers(0)
        for a, b in DIRECTIONS:
            @pl.when(inside(a))
            def _():
                pl.semaphore_signal(
                    barrier, inc=1, device_id=(1, lat + a, (lon + b + n_lon) % n_lon),
                    device_id_type=MESH,
                )
        walls = jnp.where(lat == 0, 3, 0) + jnp.where(lat == n_lat - 1, 3, 0)
        pl.semaphore_wait(barrier, peers + 8 - walls)
        for load in loads:
            load.wait()

        diag = lax.broadcasted_iota(jnp.int32, (count, count), 0) == lax.broadcasted_iota(
            jnp.int32, (count, count), 1
        )
        wet = jnp.sum(
            jnp.where(diag, covered[...].astype(jnp.float32), 0.0), axis=1, keepdims=True
        )
        sea = wet * (1 - land_v[...]).astype(jnp.float32)
        for y in range(2):
            grid[ACTIVE, y, core, main] = sea[:, y * width:(y + 1) * width]

        lane = lax.broadcasted_iota(jnp.int32, (TILE, width), 1)

        def pack(lo, num, packed):
            def body(t):
                r = pl.ds(pl.multiple_of(first + t * TILE, TILE), TILE)
                east = jnp.zeros((TILE, width), jnp.float32)
                west = east
                for c in range(num):
                    for y in range(2):
                        x = grid[lo + c, y, r, main]
                        slot = (c * 2 + y) * NSUB
                        mine = (lane >= slot) & (lane < slot + NSUB)
                        east = jnp.where(mine, pltpu.roll(x, (slot + NSUB) % width, 1), east)
                        west = jnp.where(mine, pltpu.roll(x, slot, 1) if slot else x, west)
                q = pl.ds(pl.multiple_of(t * TILE, TILE), TILE)
                packed[0, q, :] = east
                packed[1, q, :] = west
            tile_loop(count // TILE, 2, body)

        def halo(lo, num, packed, got, ssem, rsem, begin):
            for k, (a, b) in enumerate(DIRECTIONS):
                src_row = {-1: 0, 0: 0, 1: count - TILE}[a]
                dst_row = {-1: count, 0: 0, 1: -TILE}[a]
                rows = count if a == 0 else TILE
                if b == 0:
                    src = grid.at[pl.ds(lo, num), :, pl.ds(first + src_row, rows), main]
                    dst = grid.at[pl.ds(lo, num), :, pl.ds(first + dst_row, rows), main]
                else:
                    d = 0 if b > 0 else 1
                    src = packed.at[d, pl.ds(src_row, rows), :]
                    dst = got.at[d, pl.ds(TILE + dst_row, rows), :]
                copy = pltpu.make_async_remote_copy(
                    src_ref=src, dst_ref=dst, send_sem=ssem.at[k], recv_sem=rsem.at[k],
                    device_id=(1, lat + a, (lon + b + n_lon) % n_lon), device_id_type=MESH,
                )
                if begin:
                    @pl.when(inside(a))
                    def _():
                        copy.start()
                else:
                    @pl.when(inside(a))
                    def _():
                        copy.wait_send()

                    @pl.when(inside(-a))
                    def _():
                        copy.wait_recv()

        def side_of(got, slot, q):
            east = got[1, q, :]
            west = got[0, q, :]
            east = pltpu.roll(east, (width - slot) % width, 1) if slot else east
            west = pltpu.roll(west, width - NSUB - slot, 1)
            return jnp.where(
                lane < NSUB, east, jnp.where(lane >= width - NSUB, west, 0.0)
            )

        def unpack(lo, num, got, after):
            def body(t):
                q = pl.ds(pl.multiple_of(t * TILE, TILE), TILE)
                r = pl.ds(pl.multiple_of(first + (t - 1) * TILE, TILE), TILE)
                for c in range(num):
                    for y in range(2):
                        grid[lo + c, y, r, side] = side_of(got, (c * 2 + y) * NSUB, q)
                after(r)
            tile_loop(count // TILE + 2, 2, body)

        pack(0, 8, pack_early)
        halo(0, 8, pack_early, got_early, early_ssem, early_rsem, True)

        def ice_statics(r):
            for y in range(2):
                conc = grid[CONC, y, r, :]
                act = grid[ACTIVE, y, r, :]
                strength[y, r, :] = (
                    (RELAX / (1.0 + RELAX)) * grid[MASS, y, r, :] * jnp.exp(CSTAR * (conc - 1.0)) * act
                )
                dragb[y, r, :] = CW * conc * act

        wait_bytes(ids, ids_rsem)
        wanted = me * per
        row_lane = lax.broadcasted_iota(jnp.int32, (per, count), 1)
        row_sub = lax.broadcasted_iota(jnp.int32, (per, count), 0)
        mine = row_lane == row_sub + wanted
        blocks = lax.broadcasted_iota(jnp.int32, (per, count), 1).astype(jnp.float32)
        base = (me * count).astype(jnp.float32)
        for p in range(peers):
            owned = jnp.broadcast_to(ids[p], (per, count)).astype(jnp.float32)
            local = jnp.sum(jnp.where(mine, owned, 0.0), axis=1, keepdims=True) - base
            one_hot[pl.ds(p * per, per), :] = jnp.where(local == blocks, 1.0, 0.0)

        halo(0, 8, pack_early, got_early, early_ssem, early_rsem, False)
        unpack(0, 8, got_early, ice_statics)

        def east_of(x):
            return pltpu.roll(x, 2 * width - 1, 1)

        def west_of(x):
            return pltpu.roll(x, 1, 1)

        sub = lax.broadcasted_iota(jnp.int32, (TILE, 2 * width), 0)

        def next_row(x, after):
            return pltpu.roll(jnp.where(sub == 0, after, x), TILE - 1, 0)

        def last_row(x, before):
            return pltpu.roll(jnp.where(sub == TILE - 1, before, x), 1, 0)

        def sweep(g, new_stress, new_velocity):
            spots = [
                pl.ds(pl.multiple_of(first + (g * GROUP + j - 2) * TILE, TILE), TILE)
                for j in range(GROUP + 2)
            ]
            before, spots, after = spots[0], spots[1:-1], spots[-1]
            keep = 1.0 / (1.0 + RELAX)
            vels, stresses = [], []
            for r in spots:
                vels.append([(grid[U, y, r, :], grid[V, y, r, :]) for y in range(2)])
            if new_stress:
                follow = (grid[U, 0, after, :], grid[V, 0, after, :])
            for j, r in enumerate(spots):
                if not new_stress:
                    stresses.append(
                        [tuple(grid[c, y, r, :] for c in (S1, S2, S12)) for y in range(2)]
                    )
                    continue
                beyond = vels[j + 1][0] if j + 1 < GROUP else follow
                row = []
                for y in range(2):
                    u, v = vels[j][y]
                    if y == 0:
                        u_up, v_up = vels[j][1]
                    else:
                        u_up = next_row(vels[j][0][0], beyond[0])
                        v_up = next_row(vels[j][0][1], beyond[1])
                    sxx = east_of(u) - u
                    syy = v_up - v
                    shear = (u_up - u) + (east_of(v) - v)
                    div = sxx + syy
                    ten = sxx - syy
                    square = div * div + (ten * ten + shear * shear) * (1.0 / ECC2) + DMIN2
                    inverse = lax.rsqrt(square)
                    visc = strength[y, r, :] * inverse
                    s1 = grid[S1, y, r, :] * keep + visc * (div - square * inverse)
                    s2 = grid[S2, y, r, :] * keep + visc * ten * (1.0 / ECC2)
                    s12 = grid[S12, y, r, :] * keep + visc * shear * (0.5 / ECC2)
                    grid[S1, y, r, :] = s1
                    grid[S2, y, r, :] = s2
                    grid[S12, y, r, :] = s12
                    row.append((s1, s2, s12))
                stresses.append(row)
            if not new_velocity:
                return
            yy_before = 0.5 * (grid[S1, 1, before, :] - grid[S2, 1, before, :])
            cross_before = grid[S12, 1, before, :]
            for j, r in enumerate(spots):
                xx = [0.5 * (s1 + s2) for s1, s2, _ in stresses[j]]
                yy = [0.5 * (s1 - s2) for s1, s2, _ in stresses[j]]
                cross = [s12 for _, _, s12 in stresses[j]]
                yy_down = [last_row(yy[1], yy_before), yy[0]]
                cross_down = [last_row(cross[1], cross_before), cross[0]]
                yy_before, cross_before = yy[1], cross[1]
                for y in range(2):
                    u, v = vels[j][y]
                    force_x = xx[y] - west_of(xx[y]) + (cross[y] - cross_down[y])
                    force_y = cross[y] - west_of(cross[y]) + (yy[y] - yy_down[y])
                    mass = grid[MASS, y, r, :]
                    cx, cy = grid[CUR_X, y, r, :], grid[CUR_Y, y, r, :]
                    dx, dy = cx - u, cy - v
                    square = dx * dx + dy * dy + DRAG_FLOOR
                    drag = dragb[y, r, :] * (square * lax.rsqrt(square))
                    gain = grid[ACTIVE, y, r, :] / (
                        jnp.maximum(mass, MASS_FLOOR) * (1.0 / DTE) + drag
                    )
                    inertia = mass * (1.0 / DTE)
                    turn = CORIO * mass
                    grid[U, y, r, :] = gain * (
                        inertia * u + force_x + grid[PUSH_X, y, r, :] + drag * cx + turn * v
                    )
                    grid[V, y, r, :] = gain * (
                        inertia * v + force_y + grid[PUSH_Y, y, r, :] + drag * cy - turn * u
                    )

        groups = (count // TILE + 2) // GROUP

        def stress_only():
            tile_loop(groups, 1, lambda g: sweep(g, True, False))

        perm = one_hot[...].astype(jnp.bfloat16)
        stress_only()
        wait_bytes(recv.at[pl.ds(2, 4)], fwd_rsem.at[0])
        for c in range(2):
            both = split_dot(perm, recv[2 + c], (0,))
            for y in range(2):
                grid[CUR_X + c, y, core, main] = both[:, y * width:(y + 1) * width]
        pack(CUR_X, 2, pack_mid)
        halo(CUR_X, 2, pack_mid, got_mid, mid_ssem, mid_rsem, True)
        for c in range(2):
            both = split_dot(perm, recv[4 + c], (0,))
            for y in range(2):
                part = both[:, y * width:(y + 1) * width]
                grid[PUSH_X + c, y, core, main] = grid[MASS, y, core, main] * part
        wait_bytes(recv.at[pl.ds(0, 2)], fwd_rsem.at[1])
        for c in range(2):
            both = split_dot(perm, recv[c], (0,))
            for y in range(2):
                part = both[:, y * width:(y + 1) * width]
                grid[PUSH_X + c, y, core, main] = grid[ACTIVE, y, core, main] * (
                    grid[CONC, y, core, main] * part - grid[PUSH_X + c, y, core, main]
                )
        pack(PUSH_X, 2, pack_late)
        halo(PUSH_X, 2, pack_late, got_late, late_ssem, late_rsem, True)

        for y in range(2):
            share = grid[CONC, y, core, main] * grid[ACTIVE, y, core, main]
            back[2, :, pl.ds(y * width, width)] = split_dot(perm, share, (1,))
        send_rows(0, back, 2, 1, ret, 2, ret_ssem.at[0], ret_rsem.at[0])

        halo(CUR_X, 2, pack_mid, got_mid, mid_ssem, mid_rsem, False)
        unpack(CUR_X, 2, got_mid, lambda r: None)
        halo(PUSH_X, 2, pack_late, got_late, late_ssem, late_rsem, False)
        unpack(PUSH_X, 2, got_late, lambda r: None)
        tile_loop(groups, 1, lambda g: sweep(g, False, True))
        tile_loop((NSUB - 1) * groups, 1, lambda k: sweep(k % groups, True, True))

        def returned(t):
            q = pl.ds(pl.multiple_of(t * TILE, TILE), TILE)
            r = pl.ds(pl.multiple_of(first + t * TILE, TILE), TILE)
            for y in range(2):
                half = pl.ds(y * width, width)
                u, v = grid[U, y, r, main], grid[V, y, r, main]
                out[0, 0, q, half] = u
                out[0, 1, q, half] = v
                dx, dy = u - grid[CUR_X, y, r, main], v - grid[CUR_Y, y, r, main]
                drag = dragb[y, r, main] * jnp.sqrt(dx * dx + dy * dy + DRAG_FLOOR)
                forc[0, q, half] = drag * dx
                forc[1, q, half] = drag * dy

        tile_loop(count // TILE, 2, returned)
        for c in range(2):
            back[c] = split_dot(perm, forc[c], (1,))
        send_rows(0, back, 0, 2, ret, 0, ret_ssem.at[1], ret_rsem.at[1])
        wait_bytes(back.at[pl.ds(2, 1)], ret_ssem.at[0])
        wait_bytes(back.at[pl.ds(0, 2)], ret_ssem.at[1])


def per_device_kernel(n_lat, n_lon, fields, block_owner, ice_covered, land_mask):
    count, cells = land_mask.shape
    peers = n_lat * n_lon
    long = count + 2 * LEAD
    f32 = jnp.float32
    anywhere = pl.BlockSpec(memory_space=pl.ANY)
    in_vmem = pl.BlockSpec(memory_space=pltpu.VMEM)
    dma = pltpu.SemaphoreType.DMA
    return pl.pallas_call(
        functools.partial(step_kernel, n_lat, n_lon),
        out_shape=jax.ShapeDtypeStruct((1, 2, count, cells), f32),
        in_specs=[anywhere, in_vmem, in_vmem, anywhere],
        out_specs=in_vmem,
        scratch_shapes=[
            pltpu.VMEM((7, count, cells), f32),
            pltpu.VMEM((2, count, cells), f32),
            pltpu.VMEM((3, count, cells), f32),
            pltpu.VMEM((peers, 1, count), jnp.int32),
            pltpu.VMEM((6, count, cells), f32),
            pltpu.VMEM((12, 2, long, 2 * BX), f32),
            pltpu.VMEM((2, long, 2 * BX), f32),
            pltpu.VMEM((2, long, 2 * BX), f32),
            pltpu.VMEM((6, count, cells), f32),
            pltpu.VMEM((count, count), f32),
            pltpu.VMEM((3, count, cells), f32),
            pltpu.VMEM((count, cells), jnp.int32),
            pltpu.VMEM((2, count, BX), f32),
            pltpu.VMEM((2, count, BX), f32),
            pltpu.VMEM((2, count, BX), f32),
            pltpu.VMEM((2, count + 2 * TILE, BX), f32),
            pltpu.VMEM((2, count + 2 * TILE, BX), f32),
            pltpu.VMEM((2, count + 2 * TILE, BX), f32),
            dma((3,)), dma, dma, dma((2,)), dma((2,)), dma((2,)), dma((2,)),
            dma((8,)), dma((8,)), dma((8,)), dma((8,)), dma((8,)), dma((8,)),
        ],
        compiler_params=pltpu.CompilerParams(
            collective_id=0, has_side_effects=True, vmem_limit_bytes=63 * 1024 * 1024
        ),
    )(fields, block_owner.reshape(1, count), ice_covered.reshape(1, count), land_mask)


def solution(mesh):
    placed = (
        P("comp", None, ("lat", "lon"), None),
        P(("lat", "lon")),
        P(("lat", "lon")),
        P(("lat", "lon"), None),
    )
    n_lat, n_lon = mesh.shape["lat"], mesh.shape["lon"]

    def body(fields, block_owner, ice_covered, land_mask):
        count = block_owner.shape[0]
        whole_tiles = count % (n_lat * n_lon * TILE) == 0 and count == BX
        if whole_tiles and n_lon > 2:
            return per_device_kernel(n_lat, n_lon, fields, block_owner, ice_covered, land_mask)
        return per_device(fields, block_owner, ice_covered, land_mask)

    return jax.shard_map(
        body,
        mesh=mesh,
        in_specs=placed,
        out_specs=P("comp", None, ("lat", "lon"), None),
        check_vma=False,
    )
```
